128 devices in a mesh: branch: 16 (over z, x), group: 8 (over y, core).
Axes of the slice: x: 4, y: 4, z: 4, core: 2. Of those that a mesh axis runs over, the one named last changes fastest.
Arguments:
- basis: float32 [2, 131072, 256], P(None, ('branch', 'group')), may hold values from -8 to 8
- spread_owner: int32 [131072, 2], P(('branch', 'group')), may hold values from 0 to 127, all different within a row; in each aligned block of 1024 rows (0 to 1023, 1024 to 2047, ...) at most 32 rows name the same one
- spread_row: int32 [131072, 2], P(('branch', 'group')), may hold values from 0 to 1023
- spread_weight: float32 [131072, 2], P(('branch', 'group')), may hold values from 0.2 to 1
- gram_term: bfloat16 [256, 512, 512], P(('branch', 'group')), may hold values from -0.25 to 0.25
- near_block: bfloat16 [256, 8, 512, 512], P(('branch', 'group')), may hold values from -0.09375 to 0.09375
- near_list: int32 [256, 8], P(('branch', 'group')), may hold values from 0 to 1
- leaf_basis: bfloat16 [256, 64, 512], P(('branch', 'group')), may hold values from -0.25 to 0.25
- far_block: bfloat16 [256, 16, 64, 64], P(('branch', 'group')), may hold values from -0.1875 to 0.1875
- far_list: int32 [256, 16], P(('branch', 'group')), may hold values from 0 to 31
- ascend: bfloat16 [256, 64, 64], P(('branch', 'group')), may hold values from -0.125 to 0.125
- descend: bfloat16 [256, 64, 64], P(('branch', 'group')), may hold values from -0.75 to 0.75
- top_block: bfloat16 [512, 512], P('group'), may hold values from -0.25 to 0.25
Outputs:
- next_vector: float32 [131072, 256], P(('branch', 'group'))
- hessenberg: float32 [3, 256], replicated
The draws below stay inside these ranges and needn't reach their ends.
Inputs may be any that keep to these rules, and one draw needn't show every extreme that they name: `spread_owner`: within the rows of one device no owner is named by more than 32 entries, and one row never names an owner twice.
All inputs are finite; a program needn't handle non-finite values.
Results may differ from the reference program's by a relative error of at most 0.0035.
Values may be sent and summed in bfloat16 or wider, within the bound.
A program may use at most 64 MiB of HBM per device.

```python
import math
import jax
import jax.numpy as jnp
import numpy as np
from jax import lax

LEAF = 512
RANK = 64
C = 256
NEAR = 8
KFAR = 16
KRY = 2
SPREAD = 2
LEAVES = 2
ROWS_DEV = 1024
ROWS = 131072
LEAVES_ALL = 256
MOST = 32
GROUPS = 8
N_BRANCH = 16
N_GROUP = 8
DEVICES = 128


def draw_basis(key, part):
    shared_key, own_key = jax.random.split(jax.random.fold_in(key, 7), 2)
    full_shape = (KRY, ROWS, C)
    shared = jax.random.normal(shared_key, (1, ROWS, C), jnp.float32)
    own_part = jax.random.normal(own_key, full_shape, jnp.float32)
    values = 0.6 * shared + 0.8 * own_part
    return jnp.clip(values, -8.0, 8.0).astype(jnp.float32)


def touch_ends(array, key, least, top_value):
    longest = array.shape.index(max(array.shape))
    spots = []
    for shift in (0, 1):
        where = [jax.random.randint(jax.random.fold_in(key, axis), (), 0, length) for axis, length in enumerate(array.shape)]
        where[longest] = (where[longest] + shift) % array.shape[longest]
        spots.append(tuple(where))
    return array.at[spots[0]].set(least).at[spots[1]].set(top_value)


def level_of(stream_key, extent, cuts, low, top_value):
    gain = 1.0
    for axis_at, parts in cuts:
        heights = jax.random.uniform(jax.random.fold_in(jax.random.fold_in(stream_key, 6), axis_at), (parts,), jnp.float32, low / len(cuts), top_value / len(cuts))
        gain = gain * jnp.repeat(jnp.exp(heights), extent[axis_at] // parts).reshape((-1,) + (1,) * (len(extent) - 1 - axis_at))
    return gain


def routed_block(key, own, number, rows, number_of, top, reach, slope):
    order = jax.random.permutation(key, number_of)
    packed, usual = portions_of(number_of, rows * top, reach, slope, True), portions_of(number_of, rows * top, reach, slope, False)
    places = jnp.arange(number_of)

    def named(lengths, rotation):
        used = int((lengths > 0).sum())
        fixed = max(1, used // 4)
        moved = fixed + (places - fixed + rotation * (used - fixed)) % max(1, number_of - fixed)
        return jnp.zeros((number_of,), jnp.int32).at[order[jnp.where(places < fixed, places, moved)]].set(jnp.asarray(lengths, jnp.int32))

    lengths = jnp.where(number % 4 == 0, named(packed, number // 4), named(usual, number - number // 4 - 1))
    mixed = jax.random.permutation(jax.random.fold_in(own, 3), number_of)
    donor, taker = mixed[0:number_of // 2 * 2:2], mixed[1:number_of // 2 * 2:2]
    margin = jnp.minimum(lengths[donor] - 1, reach - lengths[taker]) // 2
    margin = jnp.where((donor == order[0]) | (taker == order[0]) | (lengths[taker] == 0), 0, jnp.maximum(margin, 0))
    moved = jax.random.randint(jax.random.fold_in(own, 4), (number_of // 2,), 0, 1 << 20) % (margin + 1)
    lengths = lengths.at[donor].add(-moved).at[taker].add(moved)
    items = jnp.searchsorted(jnp.cumsum(lengths), jnp.arange(rows * top), side="right").astype(jnp.int32)
    listing = items.reshape(top, rows).T
    listing = listing[jax.random.permutation(jax.random.fold_in(own, 1), rows)]
    rotation = jax.random.randint(jax.random.fold_in(own, 2), (rows, 1), 0, top)
    return jnp.take_along_axis(listing, (jnp.arange(top)[None, :] + rotation) % top, axis=1)


def portions_of(number_of, total, most, slope, full):
    portions = [(1 << 20) // math.isqrt(standing ** slope) + 1 for standing in range(1, number_of + 1)]
    largest = most if full else min(most, max(-(-total // number_of), total * portions[0] // sum(portions)))
    least = 1 if total - largest >= number_of - 1 else 0
    given, surplus = [largest] + [least] * (number_of - 1), total - largest - least * (number_of - 1)
    while surplus > 0:
        movable = [i for i in range(1, number_of) if given[i] < largest] or [i for i in range(1, number_of) if given[i] < most]
        mass, budget = sum([portions[i] for i in movable]), surplus
        for i in movable:
            more = min(most - given[i], max(1, budget * portions[i] // mass), surplus)
            given[i] = given[i] + more
            surplus = surplus - more
    return np.array(given)


def gaussian(rng, shape, scale, limit, pieces=(), held_as=jnp.bfloat16):
    drawn = scale * jax.random.normal(rng, shape, jnp.float32)
    if pieces:
        drawn = drawn * level_of(rng, shape, pieces, -0.22, 0.18)
    return jnp.clip(drawn, -limit, limit).astype(held_as)


def setup_inputs(seed: int = 0) -> dict:
    key_list = jax.random.split(jax.random.key(seed), 14)
    basis = draw_basis(jax.random.fold_in(key_list[13], 71), 0)
    spread_owner_keys = jax.random.split(jax.random.fold_in(key_list[1], 1), ROWS // ROWS_DEV)
    spread_owner_turns = jax.random.permutation(jax.random.fold_in(key_list[1], 3), ROWS // ROWS_DEV)
    spread_owner = jax.vmap(lambda own, number: routed_block(jax.random.fold_in(key_list[1], 2), own, number, ROWS_DEV, DEVICES, SPREAD, MOST, 2))(spread_owner_keys, spread_owner_turns).reshape((ROWS, SPREAD))
    spread_row = touch_ends(jax.random.randint(key_list[2], (ROWS, SPREAD), 0, ROWS_DEV), jax.random.fold_in(key_list[2], 1), 0, ROWS_DEV - 1).astype(jnp.int32)
    spread_weight = jnp.clip(0.2 + 0.8 * jax.random.uniform(key_list[3], (ROWS, SPREAD), jnp.float32) ** level_of(key_list[3], (ROWS, SPREAD), ((0, 128),), -0.2, 0.2), 0.2, 1.0)
    gram_term = gaussian(key_list[4], (LEAVES_ALL, LEAF, LEAF), LEAF ** -0.5, 0.25, ((0, 128),))
    near_block = gaussian(key_list[5], (LEAVES_ALL, NEAR, LEAF, LEAF), (LEAF * NEAR) ** -0.5, 0.09375, ((0, 128),))
    near_list = touch_ends(jax.random.randint(key_list[6], (LEAVES_ALL, NEAR), 0, LEAVES), jax.random.fold_in(key_list[6], 1), 0, LEAVES - 1).astype(jnp.int32)
    leaf_basis = gaussian(key_list[7], (LEAVES_ALL, RANK, LEAF), LEAF ** -0.5, 0.25, ((0, 128),))
    far_block = gaussian(key_list[8], (LEAVES_ALL, KFAR, RANK, RANK), (RANK * KFAR) ** -0.5, 0.1875, ((0, 128),))
    far_list = touch_ends(jax.random.randint(key_list[9], (LEAVES_ALL, KFAR), 0, N_BRANCH * LEAVES), jax.random.fold_in(key_list[9], 1), 0, (N_BRANCH * LEAVES) - 1).astype(jnp.int32)
    ascend = gaussian(key_list[10], (LEAVES_ALL, RANK, RANK), (RANK * LEAVES * N_BRANCH) ** -0.5, 0.125, ((0, 128),))
    descend = gaussian(key_list[11], (LEAVES_ALL, RANK, RANK), RANK ** -0.5, 0.75, ((0, 128),))
    top_block = gaussian(key_list[12], (GROUPS * RANK, GROUPS * RANK), (GROUPS * RANK) ** -0.5, 0.25, ((0, 8),))
    return dict(basis=basis, spread_owner=spread_owner, spread_row=spread_row, spread_weight=spread_weight, gram_term=gram_term, near_block=near_block, near_list=near_list, leaf_basis=leaf_basis, far_block=far_block, far_list=far_list, ascend=ascend, descend=descend, top_block=top_block)


HIGHEST_PRECISION = lax.Precision.HIGHEST

def product(pattern, first_op, second_op):
    return jnp.einsum(pattern, first_op.astype(jnp.float32), second_op.astype(jnp.float32), precision=HIGHEST_PRECISION)

def reference(basis, spread_owner, spread_row, spread_weight, gram_term, near_block, near_list, leaf_basis, far_block, far_list, ascend, descend, top_block):
    devices = N_BRANCH * N_GROUP
    rows_dev = LEAVES * LEAF
    columns = basis.shape[2]
    vector = basis[KRY - 1]
    target = spread_owner * rows_dev + spread_row
    dual_in = jnp.zeros((devices * rows_dev, columns), jnp.float32)
    for spread_at in range(SPREAD):
        dual_in = dual_in.at[target[:, spread_at]].add(spread_weight[:, spread_at, None] * vector)
    dual_low = dual_in.astype(jnp.bfloat16).reshape(devices, LEAVES, LEAF, columns)
    dual_split = dual_in.reshape(devices, LEAVES, LEAF, columns)
    gram_split = gram_term.reshape(devices, LEAVES, LEAF, LEAF)
    near_split = near_block.reshape(devices, LEAVES, NEAR, LEAF, LEAF)
    near_index = near_list.reshape(devices, LEAVES, NEAR)
    basis_split = leaf_basis.reshape(devices, LEAVES, RANK, LEAF)

    def upward(operands):
        dual_dev, low_dev, gram_dev, near_dev, index_dev, base_dev = operands
        first_pass = dual_dev + product('lji,ljc->lic', gram_dev, low_dev)
        first_low = first_pass.astype(jnp.bfloat16)
        near_sum = product('lkij,lkjc->lic', near_dev, first_low[index_dev])
        leaf_coeff = product('lri,lic->lrc', base_dev, first_low)
        return (first_pass, near_sum, leaf_coeff)
    first_pass, near_sum, leaf_coeff = lax.map(upward, (dual_split, dual_low, gram_split, near_split, near_index, basis_split))
    coeff_low = leaf_coeff.astype(jnp.bfloat16).reshape(N_BRANCH, N_GROUP, LEAVES, RANK, columns)
    ascend_split = ascend.reshape(N_BRANCH, N_GROUP, LEAVES, RANK, RANK)
    parent = product('bglrs,bglsc->grc', ascend_split, coeff_low)
    parent_low = parent.astype(jnp.bfloat16).reshape(N_GROUP * RANK, columns)
    top_field = jnp.dot(top_block, parent_low, preferred_element_type=jnp.float32)
    field_low = top_field.astype(jnp.bfloat16).reshape(N_GROUP, RANK, columns)
    by_group = jnp.transpose(coeff_low, (1, 0, 2, 3, 4)).reshape(N_GROUP, N_BRANCH * LEAVES, RANK, columns)
    far_split = far_block.reshape(devices, LEAVES, KFAR, RANK, RANK)
    far_index = far_list.reshape(devices, LEAVES, KFAR)
    descend_split = descend.reshape(devices, LEAVES, RANK, RANK)
    group_ids = (jnp.arange(devices, dtype=jnp.int32) % N_GROUP).astype(jnp.int32)

    def downward(operands):
        first_dev, near_dev, gram_dev, base_dev, far_dev, index_dev, desc_dev, group_id = operands
        sources = by_group[group_id][index_dev]
        far_sum = product('lkrs,lksc->lrc', far_dev, sources)
        descent = far_sum + product('lrs,sc->lrc', desc_dev, field_low[group_id])
        dual_image = first_dev + near_dev + product('lri,lrc->lic', base_dev, descent.astype(jnp.bfloat16))
        return dual_image + product('lij,ljc->lic', gram_dev, dual_image.astype(jnp.bfloat16))
    dual_out = lax.map(downward, (first_pass, near_sum, gram_split, basis_split, far_split, far_index, descend_split, group_ids))
    dual_out = dual_out.reshape(devices * rows_dev, columns)
    image_primal = jnp.zeros((devices * rows_dev, columns), jnp.float32)
    for spread_at in range(SPREAD):
        image_primal = image_primal + spread_weight[:, spread_at, None] * dual_out[target[:, spread_at]]
    total_rows = devices * rows_dev
    projection = lax.optimization_barrier(jnp.sum(basis * image_primal[None], axis=1)) / total_rows
    remainder = image_primal - lax.optimization_barrier(jnp.sum(projection[:, None, :] * basis, axis=0))
    square = lax.optimization_barrier(jnp.sum(remainder * remainder, axis=0)) / total_rows
    norm_scale = jnp.sqrt(square + 1e-06)
    return (remainder / norm_scale, jnp.concatenate([projection, norm_scale[None]], axis=0))
```

```python
import jax
import jax.numpy as jnp
from jax import lax
from jax.experimental import pallas as pl
from jax.experimental.pallas import tpu as pltpu
from jax.sharding import Mesh
from jax.sharding import PartitionSpec as P

AXES = ("branch_0", "branch_1", "group_0", "group_1")
BRANCH_GROUP = AXES
GROUP = AXES[2:]
MESH = pl.DeviceIdType.MESH
F32 = jnp.float32
BF16 = jnp.bfloat16
DEV = 128
SLOTS = 32
ROWS = 1024
LEAF = 512
RANK = 64
COLS = 256
TOTAL = DEV * ROWS
SELF = 2


def dot(a, b):
    return jnp.dot(a, b, preferred_element_type=F32)


def dot_t(a, b):
    return lax.dot_general(a, b, (((0,), (0,)), ((), ())), preferred_element_type=F32)


def kernel(
    owner_ref, row_ref, weight_ref, near_list, far_list, top_ref,
    basis_hbm, gram_hbm, near_hbm, base_hbm, far_hbm, asc_hbm, desc_hbm,
    out_ref, hess_ref,
    basis, gram, near, base, far, asc, desc,
    rank_of, weight_hi, weight_lo, row_of,
    pick_hi, pick_lo, place,
    vec_hi, vec_lo,
    send, got, reply, back,
    row_send, row_got,
    acc, first, first_low, near_sum, dual_low, image,
    ag0, ag1, coeff, far_flat, far_in,
    asc_send, asc_got, asc_flat,
    tops, sums1, sums2,
    load_sem, send_sem, got_sem, row_send_sem, row_sem, reply_sem, back_sem,
    asc_send_sem, asc_sem, ag_send_sem, ag_sem, top_send_sem, top_sem, sum_send_sem, sum_sem,
):
    z, x, y, c = (lax.axis_index(a) for a in AXES)
    zs = [z] + [lax.rem(z + d, 4) for d in (1, 2, 3)]
    xs = [x] + [lax.rem(x + d, 4) for d in (1, 2, 3)]
    ys = [y] + [lax.rem(y + d, 4) for d in (1, 2, 3)]
    cs = [c, 1 - c]
    branch = z * 4 + x
    group = y * 2 + c
    me = branch * 8 + group

    loads = [
        pltpu.make_async_copy(src, dst, load_sem.at[n])
        for n, (src, dst) in enumerate(
            (
                (basis_hbm, basis), (gram_hbm, gram), (base_hbm, base), (asc_hbm, asc),
                (desc_hbm, desc), (far_hbm, far), (near_hbm, near),
            )
        )
    ]
    for load in loads:
        load.start()

    barrier = pltpu.get_barrier_semaphore()
    for k in range(1, DEV):
        pl.semaphore_signal(
            barrier, inc=1,
            device_id=(zs[k // 32], xs[k // 8 % 4], ys[k // 2 % 4], cs[k % 2]),
            device_id_type=MESH,
        )

    owners = lax.broadcasted_iota(jnp.int32, (DEV, ROWS), 0)
    hit0 = jnp.broadcast_to(owner_ref[0:1, :], (DEV, ROWS)) == owners
    hit1 = jnp.broadcast_to(owner_ref[1:2, :], (DEV, ROWS)) == owners
    hit = jnp.where(hit0, 1.0, 0.0) + jnp.where(hit1, 1.0, 0.0)
    weight = jnp.where(
        hit0, jnp.broadcast_to(weight_ref[0:1, :], (DEV, ROWS)),
        jnp.broadcast_to(weight_ref[1:2, :], (DEV, ROWS)),
    )
    high = weight.astype(BF16).astype(F32)
    weight_hi[...] = high
    weight_lo[...] = weight - high
    row_of[...] = jnp.where(
        hit0, jnp.broadcast_to(row_ref[0:1, :], (DEV, ROWS)),
        jnp.broadcast_to(row_ref[1:2, :], (DEV, ROWS)),
    ).astype(F32)
    upto = jnp.where(
        lax.broadcasted_iota(jnp.int32, (128, 128), 0) <= lax.broadcasted_iota(jnp.int32, (128, 128), 1),
        1.0, 0.0,
    ).astype(BF16)
    before = jnp.zeros((DEV, 1), F32)
    for n in range(ROWS // 128):
        part = hit[:, n * 128 : (n + 1) * 128]
        count = dot(part.astype(BF16), upto) + before
        rank_of[:, n * 128 : (n + 1) * 128] = jnp.where(part > 0.5, count - 1.0, -1.0)
        before = count[:, 127:128]

    loads[0].wait()
    vector = basis[1]
    vec_hi[...] = vector.astype(BF16)
    vec_lo[...] = (vector - vector.astype(BF16).astype(F32)).astype(BF16)

    pl.semaphore_wait(barrier, DEV - 1)

    def offsets(i):
        return lax.rem(i + 2, 4), lax.rem(i + 2 + i // 4, 4)

    def to_group(i):
        dz, dx = offsets(i)
        return lax.rem(z + dz, 4), lax.rem(x + dx, 4)

    def from_group(i):
        dz, dx = offsets(i)
        return lax.rem(z + 4 - dz, 4) * 4 + lax.rem(x + 4 - dx, 4)

    def remote(src, dst, send_s, recv_s, to):
        pltpu.make_async_remote_copy(
            src_ref=src, dst_ref=dst, send_sem=send_s, recv_sem=recv_s, device_id=to, device_id_type=MESH
        ).start()

    def wait_for(ref, sem):
        pltpu.make_async_copy(ref, ref, sem).wait()

    slot_at = lax.broadcasted_iota(jnp.int32, (SLOTS, ROWS), 0).astype(F32)
    lane_at = lax.broadcasted_iota(jnp.int32, (8, 128), 1)

    def spread_out(buf, into, s_sem, r_sem, i, tz, tx, tb):
        for dy in (2, 1, 3, 0):
            for dc in (1, 0):
                to = tb * 8 + ys[dy] * 2 + cs[dc]
                if dy == 0 and dc == 0:

                    @pl.when(i != SELF)
                    def _():
                        remote(buf.at[to], into.at[me], s_sem, r_sem.at[i], (tz, tx, ys[dy], cs[dc]))

                    @pl.when(i == SELF)
                    def _():
                        pltpu.make_async_copy(buf.at[me], into.at[me], r_sem.at[i]).start()
                else:
                    remote(buf.at[to], into.at[me], s_sem, r_sem.at[i], (tz, tx, ys[dy], cs[dc]))

    def fill(i, carry):
        tz, tx = to_group(i)
        tb = tz * 4 + tx
        eight = pl.ds(pl.multiple_of(tb * 8, 8), 8)
        ranks, w_hi, w_lo, rows = rank_of[eight, :], weight_hi[eight, :], weight_lo[eight, :], row_of[eight, :]
        listed = jnp.full((8, 128), -1.0, F32)
        for slot in range(SLOTS):
            found = jnp.max(jnp.where(ranks == float(slot), rows, -1.0), axis=1, keepdims=True)
            listed = jnp.where(lane_at == slot, jnp.broadcast_to(found, (8, 128)), listed)
        for o in range(8):
            row_send[tb * 8 + o] = listed[o : o + 1, :]
        spread_out(row_send, row_got, row_send_sem, row_sem, i, tz, tx, tb)
        for o in range(8):
            mask = jnp.broadcast_to(ranks[o : o + 1, :], (SLOTS, ROWS)) == slot_at
            pick_hi[tb * 8 + o] = jnp.where(mask, jnp.broadcast_to(w_hi[o : o + 1, :], (SLOTS, ROWS)), 0.0).astype(BF16)
            pick_lo[tb * 8 + o] = jnp.where(mask, jnp.broadcast_to(w_lo[o : o + 1, :], (SLOTS, ROWS)), 0.0).astype(BF16)
        g_hi = pick_hi[pl.ds(tb * 8, 8)].reshape(8 * SLOTS, ROWS)
        g_lo = pick_lo[pl.ds(tb * 8, 8)].reshape(8 * SLOTS, ROWS)
        values = dot(g_hi, vec_hi[...]) + (dot(g_hi, vec_lo[...]) + dot(g_lo, vec_hi[...]))
        send[pl.ds(tb * 8, 8)] = values.astype(BF16).reshape(8, SLOTS, COLS)
        spread_out(send, got, send_sem, got_sem, i, tz, tx, tb)
        return carry

    lax.fori_loop(0, 16, fill, 0)

    loads[3].wait()
    own = jnp.concatenate([asc[0], asc[1]], axis=1)
    asc_send[...] = own
    for k in range(1, 16):
        remote(asc_send, asc_got.at[branch], asc_send_sem, asc_sem, (zs[k // 4], xs[k % 4], y, c))
    asc_got[branch] = own

    v0, v1 = basis[0], basis[1]
    mutual = [jnp.sum(a * b, axis=0, keepdims=True) for a, b in ((v0, v0), (v0, v1), (v1, v1))]

    loads[5].wait()
    for leaf in range(2):
        for k in range(8):
            far_flat[leaf, :, k * 128 : (k + 1) * 128] = jnp.concatenate(
                [far[leaf, 2 * k], far[leaf, 2 * k + 1]], axis=1
            )

    acc[...] = jnp.zeros_like(acc)
    row_at = lax.broadcasted_iota(jnp.int32, (SLOTS, ROWS), 1).astype(F32)

    def gather(i, carry):
        sb = from_group(i)
        wait_for(row_got.at[pl.ds(0, 8)], row_sem.at[i])
        listed = jnp.concatenate([row_got[sb * 8 + o] for o in range(8)], axis=0)
        turned = jnp.transpose(listed)
        for o in range(8):
            rows = jnp.broadcast_to(turned[0:SLOTS, o : o + 1], (SLOTS, ROWS))
            place[sb * 8 + o] = jnp.where(rows == row_at, 1.0, 0.0).astype(BF16)
        wait_for(got.at[pl.ds(0, 8)], got_sem.at[i])
        chosen = place[pl.ds(sb * 8, 8)].reshape(8 * SLOTS, ROWS)
        acc[...] += dot_t(chosen, got[pl.ds(sb * 8, 8)].reshape(8 * SLOTS, COLS))
        return carry

    lax.fori_loop(0, 16, gather, 0)

    loads[1].wait()
    loads[2].wait()
    for leaf, (slots, i, j) in enumerate(((ag0, z, x), (ag1, x, z))):
        rows = pl.ds(leaf * LEAF, LEAF)
        dual = acc[rows, :]
        passed = dual + dot_t(gram[leaf], dual.astype(BF16))
        first[rows, :] = passed
        first_low[leaf] = passed.astype(BF16)
        slots[i, j] = dot(base[leaf], first_low[leaf]).astype(BF16)
    for d in (1, 3, 2):
        remote(ag0.at[z, x], ag0.at[z, x], ag_send_sem.at[0], ag_sem.at[0], (z, xs[d], y, c))
        remote(ag1.at[x, z], ag1.at[x, z], ag_send_sem.at[1], ag_sem.at[1], (zs[d], x, y, c))

    loads[6].wait()
    near_sum[...] = jnp.zeros_like(near_sum)

    def near_of(leaf):
        def step(k, carry):
            rows = pl.ds(leaf * LEAF, LEAF)
            near_sum[rows, :] += dot(near[leaf, k], first_low[near_list[leaf, k]])
            return carry

        lax.fori_loop(0, 8, step, 0)

    near_of(0)
    three = pl.ds(0, 3)
    wait_for(ag0.at[0, three], ag_sem.at[0])
    wait_for(ag1.at[0, three], ag_sem.at[1])
    for d in (1, 3, 2):
        remote(ag0.at[z], ag0.at[z], ag_send_sem.at[2], ag_sem.at[2], (zs[d], x, y, c))
        remote(ag1.at[x], ag1.at[x], ag_send_sem.at[3], ag_sem.at[3], (z, xs[d], y, c))
    near_of(1)
    wait_for(asc_got.at[pl.ds(0, 15)], asc_sem)
    for b in range(16):
        asc_flat[:, b * 128 : (b + 1) * 128] = asc_got[b]
    wait_for(ag0.at[three], ag_sem.at[2])
    wait_for(ag1.at[three], ag_sem.at[3])
    for b in range(16):
        coeff[2 * b] = ag0[b // 4, b % 4]
        coeff[2 * b + 1] = ag1[b % 4, b // 4]
    tops[group] = dot(asc_flat[...], coeff[...].reshape(32 * RANK, COLS)).astype(BF16)
    for k in range(1, 8):
        remote(tops.at[group], tops.at[group], top_send_sem, top_sem, (z, x, ys[k // 2], cs[k % 2]))
    for leaf in range(2):
        for k in range(16):
            far_in[leaf, k * RANK : (k + 1) * RANK, :] = coeff[far_list[leaf, k]]
    far_sum = [dot(far_flat[leaf], far_in[leaf]) for leaf in range(2)]
    loads[4].wait()
    wait_for(tops.at[pl.ds(0, 7)], top_sem)
    field = dot(top_ref[...], tops[...].reshape(8 * RANK, COLS)).astype(BF16)
    for leaf in range(2):
        rows = pl.ds(leaf * LEAF, LEAF)
        descent = (far_sum[leaf] + dot(desc[leaf], field)).astype(BF16)
        dual = first[rows, :] + near_sum[rows, :] + dot_t(base[leaf], descent)
        dual_low[rows, :] = (dual + dot(gram[leaf], dual.astype(BF16))).astype(BF16)

    def answer(i, carry):
        tz, tx = to_group(i)
        tb = tz * 4 + tx
        chosen = place[pl.ds(tb * 8, 8)].reshape(8 * SLOTS, ROWS)
        reply[pl.ds(tb * 8, 8)] = dot(chosen, dual_low[...]).astype(BF16).reshape(8, SLOTS, COLS)
        spread_out(reply, back, reply_sem, back_sem, i, tz, tx, tb)
        return carry

    lax.fori_loop(0, 16, answer, 0)

    image[...] = jnp.zeros_like(image)

    def collect(i, carry):
        sb = from_group(i)
        wait_for(back.at[pl.ds(0, 8)], back_sem.at[i])
        values = back[pl.ds(sb * 8, 8)].reshape(8 * SLOTS, COLS)
        g_hi = pick_hi[pl.ds(sb * 8, 8)].reshape(8 * SLOTS, ROWS)
        g_lo = pick_lo[pl.ds(sb * 8, 8)].reshape(8 * SLOTS, ROWS)
        image[...] += dot_t(g_hi, values) + dot_t(g_lo, values)
        return carry

    lax.fori_loop(0, 16, collect, 0)

    found = image[...]
    cross = [jnp.sum(basis[k] * found, axis=0, keepdims=True) for k in range(2)]
    whole = jnp.sum(found * found, axis=0, keepdims=True)
    sums1[group] = jnp.concatenate(cross + [whole] + mutual + [jnp.zeros((2, COLS), F32)], axis=0)
    for k in range(1, 8):
        remote(sums1.at[group], sums1.at[group], sum_send_sem.at[0], sum_sem.at[0], (z, x, ys[k // 2], cs[k % 2]))
    wait_for(sums1.at[pl.ds(0, 7)], sum_sem.at[0])
    sums2[branch] = jnp.sum(sums1[...], axis=0)
    for k in range(1, 16):
        remote(sums2.at[branch], sums2.at[branch], sum_send_sem.at[1], sum_sem.at[1], (zs[k // 4], xs[k % 4], y, c))
    wait_for(sums2.at[pl.ds(0, 15)], sum_sem.at[1])
    total = jnp.sum(sums2[...], axis=0) * (1.0 / TOTAL)
    p0, p1, sq = total[0:1], total[1:2], total[2:3]
    m00, m01, m11 = total[3:4], total[4:5], total[5:6]
    square = sq - 2.0 * (p0 * p0 + p1 * p1) + (p0 * p0 * m00 + 2.0 * (p0 * p1) * m01 + p1 * p1 * m11)
    norm = jnp.sqrt(square + 1e-6)
    hess_ref[...] = jnp.concatenate([p0, p1, norm], axis=0)
    scale = 1.0 / norm
    out_ref[...] = (image[...] - (p0 * basis[0] + p1 * basis[1])) * scale

    wait_for(row_send.at[pl.ds(0, DEV - 1)], row_send_sem)
    wait_for(send.at[pl.ds(0, DEV - 1)], send_sem)
    wait_for(reply.at[pl.ds(0, DEV - 1)], reply_sem)
    wait_for(asc_got.at[pl.ds(0, 15)], asc_send_sem)
    wait_for(ag0.at[0, three], ag_send_sem.at[0])
    wait_for(ag1.at[0, three], ag_send_sem.at[1])
    wait_for(ag0.at[three], ag_send_sem.at[2])
    wait_for(ag1.at[three], ag_send_sem.at[3])
    wait_for(tops.at[pl.ds(0, 7)], top_send_sem)
    wait_for(sums1.at[pl.ds(0, 7)], sum_send_sem.at[0])
    wait_for(sums2.at[pl.ds(0, 15)], sum_send_sem.at[1])


def body(
    basis, spread_owner, spread_row, spread_weight, gram_term, near_block, near_list,
    leaf_basis, far_block, far_list, ascend, descend, top_block,
):
    vmem = pl.BlockSpec(memory_space=pltpu.VMEM)
    smem = pl.BlockSpec(memory_space=pltpu.SMEM)
    hbm = pl.BlockSpec(memory_space=pl.ANY)
    dma = pltpu.SemaphoreType.DMA
    V = pltpu.VMEM
    return tuple(
        pl.pallas_call(
            kernel,
            out_shape=(
                jax.ShapeDtypeStruct((ROWS, COLS), F32),
                jax.ShapeDtypeStruct((3, COLS), F32),
            ),
            in_specs=[vmem] * 3 + [smem] * 2 + [vmem] + [hbm] * 7,
            out_specs=(vmem, vmem),
            scratch_shapes=[
                V((2, ROWS, COLS), F32), V((2, LEAF, LEAF), BF16), V((2, 8, LEAF, LEAF), BF16),
                V((2, RANK, LEAF), BF16), V((2, 16, RANK, RANK), BF16), V((2, RANK, RANK), BF16),
                V((2, RANK, RANK), BF16),
                V((DEV, ROWS), F32), V((DEV, ROWS), F32), V((DEV, ROWS), F32), V((DEV, ROWS), F32),
                V((DEV, SLOTS, ROWS), BF16), V((DEV, SLOTS, ROWS), BF16), V((DEV, SLOTS, ROWS), BF16),
                V((ROWS, COLS), BF16), V((ROWS, COLS), BF16),
                V((DEV, SLOTS, COLS), BF16), V((DEV, SLOTS, COLS), BF16),
                V((DEV, SLOTS, COLS), BF16), V((DEV, SLOTS, COLS), BF16),
                V((DEV, 1, 128), F32), V((DEV, 1, 128), F32),
                V((ROWS, COLS), F32), V((ROWS, COLS), F32), V((2, LEAF, COLS), BF16),
                V((ROWS, COLS), F32), V((ROWS, COLS), BF16), V((ROWS, COLS), F32),
                V((4, 4, RANK, COLS), BF16), V((4, 4, RANK, COLS), BF16), V((32, RANK, COLS), BF16),
                V((2, RANK, 16 * RANK), BF16), V((2, 16 * RANK, COLS), BF16),
                V((RANK, 2 * RANK), BF16), V((16, RANK, 2 * RANK), BF16), V((RANK, 32 * RANK), BF16),
                V((8, RANK, COLS), BF16), V((8, 8, COLS), F32), V((16, 8, COLS), F32),
                dma((7,)), dma, dma((16,)), dma, dma((16,)), dma, dma((16,)),
                dma, dma, dma((4,)), dma((4,)), dma, dma, dma((2,)), dma((2,)),
            ],
            compiler_params=pltpu.CompilerParams(
                collective_id=0, has_side_effects=True, vmem_limit_bytes=67_000_000
            ),
            name="dual_step",
        )(
            spread_owner.T, spread_row.T, spread_weight.T, near_list, far_list, top_block,
            basis, gram_term, near_block, leaf_basis, far_block, ascend, descend,
        )
    )


def solution(mesh):
    finer = Mesh(mesh.devices.reshape(4, 4, 4, 2), AXES)
    split = P(BRANCH_GROUP)
    return jax.shard_map(
        body,
        mesh=finer,
        in_specs=(
            P(None, BRANCH_GROUP, None), split, split, split, split, split, split,
            split, split, split, split, split, P(GROUP, None),
        ),
        out_specs=(P(BRANCH_GROUP, None), P()),
        check_vma=False,
    )
```

```python
import jax
import jax.numpy as jnp
from jax import lax
from jax.experimental import pallas as pl
from jax.experimental.pallas import tpu as pltpu
from jax.sharding import Mesh
from jax.sharding import PartitionSpec as P

AXES = ("branch_0", "branch_1", "group_0", "group_1")
BRANCH_GROUP = AXES
GROUP = AXES[2:]
MESH = pl.DeviceIdType.MESH
F32 = jnp.float32
BF16 = jnp.bfloat16
DEV = 128
SLOTS = 32
ROWS = 1024
LEAF = 512
RANK = 64
COLS = 256
TOTAL = DEV * ROWS
SELF = 2
PARTS = 2
WIDE = COLS // PARTS


def dot(a, b):
    return jnp.dot(a, b, preferred_element_type=F32)


def dot_t(a, b):
    return lax.dot_general(a, b, (((0,), (0,)), ((), ())), preferred_element_type=F32)


def kernel(
    owner_ref, row_ref, weight_ref, near_list, far_list, top_ref,
    basis_hbm, gram_hbm, near_hbm, base_hbm, far_hbm, asc_hbm, desc_hbm,
    image_hbm, total_ref,
    basis, gram, near, base, far, asc, desc,
    rank_of, rank_low, weight_of, row_of, count_of,
    pick, place, slot_weight, slot_low, vec,
    send, got, reply, back,
    row_send, row_got,
    acc, first, first_low, near_sum, dual_two, image, image_out,
    ag0, ag1, coeff, far_flat, far_in,
    par1, par2, tops, sums1, sums2,
    load_sem, send_sem, got_sem, row_send_sem, row_sem, reply_sem, back_sem,
    ag_send_sem, ag_sem, par_send_sem, par_sem, top_send_sem, top_sem, sum_send_sem, sum_sem, out_sem,
):
    z, x, y, c = (lax.axis_index(a) for a in AXES)
    zs = [z] + [lax.rem(z + d, 4) for d in (1, 2, 3)]
    xs = [x] + [lax.rem(x + d, 4) for d in (1, 2, 3)]
    ys = [y] + [lax.rem(y + d, 4) for d in (1, 2, 3)]
    cs = [c, 1 - c]
    branch = z * 4 + x
    group = y * 2 + c
    me = branch * 8 + group

    def remote(src, dst, send_s, recv_s, to):
        pltpu.make_async_remote_copy(
            src_ref=src, dst_ref=dst, send_sem=send_s, recv_sem=recv_s, device_id=to, device_id_type=MESH
        ).start()

    def wait_for(ref, sem):
        pltpu.make_async_copy(ref, ref, sem).wait()

    barrier = pltpu.get_barrier_semaphore()
    for k in range(1, DEV):
        pl.semaphore_signal(
            barrier, inc=1,
            device_id=(zs[k // 32], xs[k // 8 % 4], ys[k // 2 % 4], cs[k % 2]),
            device_id_type=MESH,
        )

    loads = [
        pltpu.make_async_copy(src, dst, load_sem.at[n])
        for n, (src, dst) in enumerate(
            (
                (basis_hbm.at[1], basis.at[1]), (basis_hbm.at[0], basis.at[0]), (gram_hbm, gram),
                (base_hbm, base), (asc_hbm, asc), (desc_hbm, desc), (far_hbm, far), (near_hbm, near),
            )
        )
    ]
    for load in loads:
        load.start()

    owners = lax.broadcasted_iota(jnp.int32, (DEV, ROWS), 0)
    hit0 = jnp.broadcast_to(owner_ref[0:1, :], (DEV, ROWS)) == owners
    hit1 = jnp.broadcast_to(owner_ref[1:2, :], (DEV, ROWS)) == owners
    hit = jnp.where(hit0, 1.0, 0.0) + jnp.where(hit1, 1.0, 0.0)
    weight_of[...] = jnp.where(
        hit0, jnp.broadcast_to(weight_ref[0:1, :], (DEV, ROWS)),
        jnp.broadcast_to(weight_ref[1:2, :], (DEV, ROWS)),
    )
    row_of[...] = jnp.where(
        hit0, jnp.broadcast_to(row_ref[0:1, :], (DEV, ROWS)),
        jnp.broadcast_to(row_ref[1:2, :], (DEV, ROWS)),
    ).astype(F32)
    upto = jnp.where(
        lax.broadcasted_iota(jnp.int32, (128, 128), 0) <= lax.broadcasted_iota(jnp.int32, (128, 128), 1),
        1.0, 0.0,
    ).astype(BF16)
    before = jnp.zeros((DEV, 1), F32)
    for n in range(ROWS // 128):
        part = hit[:, n * 128 : (n + 1) * 128]
        count = dot(part.astype(BF16), upto) + before
        rank_of[:, n * 128 : (n + 1) * 128] = jnp.where(part > 0.5, count - 1.0, -1.0)
        before = count[:, 127:128]
    count_of[...] = jnp.broadcast_to(before, (DEV, 128))
    rank_low[...] = jnp.where(rank_of[...] >= 0.0, rank_of[...] + jnp.broadcast_to(before, (DEV, ROWS)), -1.0)

    loads[0].wait()
    vector = basis[1]
    vec[:, 0:COLS] = vector.astype(BF16)
    vec[:, COLS:] = (vector - vector.astype(BF16).astype(F32)).astype(BF16)

    def offsets(i):
        return lax.rem(i + 2, 4), lax.rem(i + 2 + i // 4, 4)

    def to_group(i):
        dz, dx = offsets(i)
        return lax.rem(z + dz, 4), lax.rem(x + dx, 4)

    def from_group(i):
        dz, dx = offsets(i)
        return lax.rem(z + 4 - dz, 4) * 4 + lax.rem(x + 4 - dx, 4)

    def spread_out(buf, into, s_sem, r_sem, i):
        tz, tx = to_group(i)
        tb = tz * 4 + tx
        for dy in (2, 1, 3, 0):
            for dc in (1, 0):
                to = tb * 8 + ys[dy] * 2 + cs[dc]
                if dy == 0 and dc == 0:

                    @pl.when(i != SELF)
                    def _():
                        remote(buf.at[to], into.at[me], s_sem, r_sem.at[i], (tz, tx, ys[dy], cs[dc]))

                    @pl.when(i == SELF)
                    def _():
                        pltpu.make_async_copy(buf.at[me], into.at[me], r_sem.at[i]).start()
                else:
                    remote(buf.at[to], into.at[me], s_sem, r_sem.at[i], (tz, tx, ys[dy], cs[dc]))

    slot_at = lax.broadcasted_iota(jnp.int32, (SLOTS, ROWS), 0).astype(F32)
    slot_col = lax.broadcasted_iota(jnp.int32, (SLOTS, COLS), 0).astype(F32)
    lane_at = lax.broadcasted_iota(jnp.int32, (SLOTS, 128), 1)

    def fill(i, carry):
        tz, tx = to_group(i)
        tb = tz * 4 + tx
        eight = pl.ds(pl.multiple_of(tb * 8, 8), 8)
        ranks, lows, weights, rows = rank_of[eight, :], rank_low[eight, :], weight_of[eight, :], row_of[eight, :]
        counts = count_of[eight, :]
        listed = jnp.zeros((SLOTS, 128), F32)
        scales = []
        for o in range(8):
            mask = (jnp.broadcast_to(ranks[o : o + 1, :], (SLOTS, ROWS)) == slot_at) | (
                jnp.broadcast_to(lows[o : o + 1, :], (SLOTS, ROWS)) == slot_at
            )
            pick[tb * 8 + o] = jnp.where(mask, 1.0, 0.0).astype(BF16)
            scale = jnp.sum(
                jnp.where(mask, jnp.broadcast_to(weights[o : o + 1, :], (SLOTS, ROWS)), 0.0), axis=1, keepdims=True
            )
            row = jnp.sum(
                jnp.where(mask, jnp.broadcast_to(rows[o : o + 1, :], (SLOTS, ROWS)), 0.0), axis=1, keepdims=True
            )
            row = jnp.broadcast_to(row, (SLOTS, 128)) + jnp.where(
                slot_col[:, 0:128] >= jnp.broadcast_to(counts[o : o + 1, :], (SLOTS, 128)), float(ROWS), 0.0
            )
            listed = jnp.where(lane_at == o, row, listed)
            slot_weight[tb * 8 + o] = jnp.broadcast_to(scale, (SLOTS, 128))
            scales.append(jnp.broadcast_to(scale, (SLOTS, COLS)))
        turned = jnp.transpose(listed)
        for o in range(8):
            row_send[tb * 8 + o, :, 0:SLOTS] = turned[o : o + 1, :]

        values = dot(pick[pl.ds(tb * 8, 8)].reshape(8 * SLOTS, ROWS), vec[...])
        for o in range(8):
            part = values[o * SLOTS : (o + 1) * SLOTS, :]
            part = (part[:, 0:COLS] + part[:, COLS:]) * scales[o]
            high = part.astype(BF16).astype(F32)
            count = jnp.broadcast_to(counts[o : o + 1, 0:1], (SLOTS, COLS))
            sent = jnp.where(slot_col >= count, part - high, high).astype(BF16)
            for p in range(PARTS):
                send[p, tb * 8 + o] = sent[:, p * WIDE : (p + 1) * WIDE]

        @pl.when(i == 0)
        def _():
            pl.semaphore_wait(barrier, DEV - 1)

        spread_out(row_send, row_got, row_send_sem, row_sem, i)
        spread_out(send.at[0], got.at[0], send_sem.at[0], got_sem.at[0], i)
        return carry

    lax.fori_loop(0, 16, fill, 0)

    def fill_rest(i, carry):
        spread_out(send.at[1], got.at[1], send_sem.at[1], got_sem.at[1], i)
        return carry

    lax.fori_loop(0, 16, fill_rest, 0)

    loads[1].wait()
    v0, v1 = basis[0], basis[1]
    mutual = [jnp.sum(a * b, axis=0, keepdims=True) for a, b in ((v0, v0), (v0, v1), (v1, v1))]

    for n in range(2, 8):
        loads[n].wait()
    for leaf in range(2):
        for k in range(8):
            far_flat[leaf, :, k * 128 : (k + 1) * 128] = jnp.concatenate(
                [far[leaf, 2 * k], far[leaf, 2 * k + 1]], axis=1
            )

    acc[...] = jnp.zeros_like(acc)
    near_sum[...] = jnp.zeros_like(near_sum)
    image[...] = jnp.zeros_like(image)
    row_at = lax.broadcasted_iota(jnp.int32, (SLOTS, ROWS), 1).astype(F32)

    def find_places(i, carry):
        sb = from_group(i)
        wait_for(row_got.at[pl.ds(0, 8)], row_sem.at[i])
        turned = jnp.transpose(jnp.concatenate([row_got[sb * 8 + o] for o in range(8)], axis=0))
        for o in range(8):
            row = turned[0:SLOTS, o : o + 1]
            low = row >= float(ROWS)
            slot_low[sb * 8 + o] = jnp.broadcast_to(jnp.where(low, 1.0, 0.0), (SLOTS, 128))
            row = jnp.where(low, row - float(ROWS), row)
            place[sb * 8 + o] = jnp.where(jnp.broadcast_to(row, (SLOTS, ROWS)) == row_at, 1.0, 0.0).astype(BF16)
        return carry

    def gather(p, start, stop):
        def step(i, carry):
            sb = from_group(i)
            wait_for(got.at[p, pl.ds(0, 8)], got_sem.at[p, i])
            chosen = place[pl.ds(sb * 8, 8)].reshape(8 * SLOTS, ROWS)
            acc[p] += dot_t(chosen, got[p, pl.ds(sb * 8, 8)].reshape(8 * SLOTS, WIDE))
            return carry

        lax.fori_loop(start, stop, step, 0)

    half = RANK // 2

    def early(p):
        partial = jnp.zeros((RANK, WIDE), F32)
        for leaf, (slots, i, j) in enumerate(((ag0, z, x), (ag1, x, z))):
            rows = pl.ds(leaf * LEAF, LEAF)
            dual = acc[p, rows, :]
            passed = dual + dot_t(gram[leaf], dual.astype(BF16))
            first[p, rows, :] = passed
            first_low[p, leaf] = passed.astype(BF16)
            low = dot(base[leaf], first_low[p, leaf]).astype(BF16)
            slots[p, i, j] = low
            partial = partial + dot(asc[leaf], low)
        par1[p, 0, x] = partial[0:half].astype(BF16)
        par1[p, 1, z] = partial[half:].astype(BF16)
        for d in (1, 3, 2):
            remote(par1.at[p, 0, x], par1.at[p, 0, x], par_send_sem.at[p, 0], par_sem.at[p, 0], (z, xs[d], y, c))
            remote(par1.at[p, 1, z], par1.at[p, 1, z], par_send_sem.at[p, 1], par_sem.at[p, 1], (zs[d], x, y, c))
        for d in (1, 3, 2):
            remote(ag0.at[p, z, x], ag0.at[p, z, x], ag_send_sem.at[p, 0], ag_sem.at[p, 0], (z, xs[d], y, c))
            remote(ag1.at[p, x, z], ag1.at[p, x, z], ag_send_sem.at[p, 1], ag_sem.at[p, 1], (zs[d], x, y, c))

    def near_of(p, leaf):
        def step(k, carry):
            rows = pl.ds(leaf * LEAF, LEAF)
            near_sum[p, rows, :] += dot(near[leaf, k], first_low[p, near_list[leaf, k]])
            return carry

        lax.fori_loop(0, 8, step, 0)

    three = pl.ds(0, 3)

    def summed(ref):
        return ((ref[0].astype(F32) + ref[1].astype(F32)) + (ref[2].astype(F32) + ref[3].astype(F32))).astype(BF16)

    def mid_a(p):
        wait_for(par1.at[p, 0, three], par_sem.at[p, 0])
        wait_for(par1.at[p, 1, three], par_sem.at[p, 1])
        par2[p, 0, z] = summed(par1.at[p, 0])
        par2[p, 1, x] = summed(par1.at[p, 1])
        for d in (1, 3, 2):
            remote(par2.at[p, 0, z], par2.at[p, 0, z], par_send_sem.at[p, 2], par_sem.at[p, 2], (zs[d], x, y, c))
            remote(par2.at[p, 1, x], par2.at[p, 1, x], par_send_sem.at[p, 3], par_sem.at[p, 3], (z, xs[d], y, c))
        wait_for(ag0.at[p, 0, three], ag_sem.at[p, 0])
        wait_for(ag1.at[p, 0, three], ag_sem.at[p, 1])
        for d in (1, 3, 2):
            remote(ag0.at[p, z], ag0.at[p, z], ag_send_sem.at[p, 2], ag_sem.at[p, 2], (zs[d], x, y, c))
            remote(ag1.at[p, x], ag1.at[p, x], ag_send_sem.at[p, 3], ag_sem.at[p, 3], (z, xs[d], y, c))

    def mid_b(p):
        wait_for(par2.at[p, 0, three], par_sem.at[p, 2])
        wait_for(par2.at[p, 1, three], par_sem.at[p, 3])
        tops[p, group, 0:half] = summed(par2.at[p, 0])
        tops[p, group, half:] = summed(par2.at[p, 1])
        for k in range(1, 8):
            remote(tops.at[p, group], tops.at[p, group], top_send_sem.at[p], top_sem.at[p], (z, x, ys[k // 2], cs[k % 2]))

    def mid_c(p):
        wait_for(tops.at[p, pl.ds(0, 7)], top_sem.at[p])
        field = dot(top_ref[...], tops[p].reshape(8 * RANK, WIDE)).astype(BF16)
        wait_for(ag0.at[p, three], ag_sem.at[p, 2])
        wait_for(ag1.at[p, three], ag_sem.at[p, 3])
        for b in range(16):
            coeff[2 * b] = ag0[p, b // 4, b % 4]
            coeff[2 * b + 1] = ag1[p, b % 4, b // 4]
        for leaf in range(2):
            for k in range(16):
                far_in[k * RANK : (k + 1) * RANK, :] = coeff[far_list[leaf, k]]
            rows = pl.ds(leaf * LEAF, LEAF)
            descent = (dot(far_flat[leaf], far_in[...]) + dot(desc[leaf], field)).astype(BF16)
            dual = first[p, rows, :] + near_sum[p, rows, :] + dot_t(base[leaf], descent)
            dual = dual + dot(gram[leaf], dual.astype(BF16))
            dual_two[p, rows, 0:WIDE] = dual.astype(BF16)
            dual_two[p, rows, WIDE:] = (dual - dual.astype(BF16).astype(F32)).astype(BF16)

    def answer(p, start, stop):
        def step(i, carry):
            tz, tx = to_group(i)
            eight = pl.ds((tz * 4 + tx) * 8, 8)
            both = dot(place[eight].reshape(8 * SLOTS, ROWS), dual_two[p])
            low = slot_low[eight].reshape(8 * SLOTS, 128) > 0.5
            reply[p, eight] = jnp.where(low, both[:, WIDE:], both[:, 0:WIDE]).astype(BF16).reshape(8, SLOTS, WIDE)
            spread_out(reply.at[p], back.at[p], reply_sem.at[p], back_sem.at[p], i)
            return carry

        lax.fori_loop(start, stop, step, 0)

    def collect(p):
        def step(i, carry):
            eight = pl.ds(from_group(i) * 8, 8)
            wait_for(back.at[p, pl.ds(0, 8)], back_sem.at[p, i])
            values = back[p, eight].reshape(8 * SLOTS, WIDE).astype(F32) * slot_weight[eight].reshape(8 * SLOTS, 128)
            high = values.astype(BF16)
            two = jnp.concatenate([high, (values - high.astype(F32)).astype(BF16)], axis=1)
            both = dot_t(pick[eight].reshape(8 * SLOTS, ROWS), two)
            image[p] += both[:, 0:WIDE] + both[:, WIDE:]
            return carry

        lax.fori_loop(0, 16, step, 0)

    lax.fori_loop(0, 16, find_places, 0)
    gather(0, 0, 16)
    early(0)
    near_of(0, 0)
    near_of(0, 1)
    gather(1, 0, 12)
    mid_a(0)
    gather(1, 12, 16)
    early(1)
    mid_b(0)
    near_of(1, 0)
    mid_a(1)
    mid_c(0)
    answer(0, 0, 8)
    mid_b(1)
    answer(0, 8, 16)
    near_of(1, 1)
    mid_c(1)
    answer(1, 0, 16)
    collect(0)
    collect(1)

    found = jnp.concatenate([image[0], image[1]], axis=1)
    image_out[...] = found
    cross = [jnp.sum(basis[k] * found, axis=0, keepdims=True) for k in range(2)]
    whole = jnp.sum(found * found, axis=0, keepdims=True)
    sums1[group] = jnp.concatenate(cross + [whole] + mutual + [jnp.zeros((2, COLS), F32)], axis=0)
    for k in range(1, 8):
        remote(sums1.at[group], sums1.at[group], sum_send_sem.at[0], sum_sem.at[0], (z, x, ys[k // 2], cs[k % 2]))
    leave = pltpu.make_async_copy(image_out, image_hbm, out_sem)
    leave.start()
    wait_for(sums1.at[pl.ds(0, 7)], sum_sem.at[0])
    sums2[branch] = jnp.sum(sums1[...], axis=0)
    for k in range(1, 16):
        remote(sums2.at[branch], sums2.at[branch], sum_send_sem.at[1], sum_sem.at[1], (zs[k // 4], xs[k % 4], y, c))
    wait_for(row_send.at[pl.ds(0, DEV - 1)], row_send_sem)
    for p in range(PARTS):
        wait_for(send.at[p, pl.ds(0, DEV - 1)], send_sem.at[p])
        wait_for(reply.at[p, pl.ds(0, DEV - 1)], reply_sem.at[p])
        wait_for(ag0.at[p, 0, three], ag_send_sem.at[p, 0])
        wait_for(ag1.at[p, 0, three], ag_send_sem.at[p, 1])
        wait_for(ag0.at[p, three], ag_send_sem.at[p, 2])
        wait_for(ag1.at[p, three], ag_send_sem.at[p, 3])
        for n in range(4):
            wait_for(par1.at[p, 0, three], par_send_sem.at[p, n])
        wait_for(tops.at[p, pl.ds(0, 7)], top_send_sem.at[p])
    leave.wait()
    wait_for(sums1.at[pl.ds(0, 7)], sum_send_sem.at[0])
    wait_for(sums2.at[pl.ds(0, 15)], sum_sem.at[1])
    wait_for(sums2.at[pl.ds(0, 15)], sum_send_sem.at[1])
    total = jnp.sum(sums2[...], axis=0) * (1.0 / TOTAL)
    p0, p1, sq = total[0:1], total[1:2], total[2:3]
    m00, m01, m11 = total[3:4], total[4:5], total[5:6]
    square = sq - 2.0 * (p0 * p0 + p1 * p1) + (p0 * p0 * m00 + 2.0 * (p0 * p1) * m01 + p1 * p1 * m11)
    norm = jnp.sqrt(square + 1e-6)
    total_ref[...] = jnp.concatenate([p0, p1, norm, 1.0 / norm, jnp.zeros((4, COLS), F32)], axis=0)


def finish(total_ref, basis_ref, image_ref, out_ref, hess_ref):
    p0, p1, scale = total_ref[0:1], total_ref[1:2], total_ref[3:4]
    out_ref[...] = (image_ref[...] - (p0 * basis_ref[0] + p1 * basis_ref[1])) * scale
    hess_ref[...] = total_ref[0:3]


def body(
    basis, spread_owner, spread_row, spread_weight, gram_term, near_block, near_list,
    leaf_basis, far_block, far_list, ascend, descend, top_block,
):
    vmem = pl.BlockSpec(memory_space=pltpu.VMEM)
    smem = pl.BlockSpec(memory_space=pltpu.SMEM)
    hbm = pl.BlockSpec(memory_space=pl.ANY)
    dma = pltpu.SemaphoreType.DMA
    V = pltpu.VMEM
    image, total = pl.pallas_call(
        kernel,
        out_shape=(
            jax.ShapeDtypeStruct((ROWS, COLS), F32),
            jax.ShapeDtypeStruct((8, COLS), F32),
        ),
        in_specs=[vmem] * 3 + [smem] * 2 + [vmem] + [hbm] * 7,
        out_specs=(hbm, vmem),
        scratch_shapes=[
            V((2, ROWS, COLS), F32), V((2, LEAF, LEAF), BF16), V((2, 8, LEAF, LEAF), BF16),
            V((2, RANK, LEAF), BF16), V((2, 16, RANK, RANK), BF16), V((2, RANK, RANK), BF16),
            V((2, RANK, RANK), BF16),
            V((DEV, ROWS), F32), V((DEV, ROWS), F32), V((DEV, ROWS), F32), V((DEV, ROWS), F32), V((DEV, 128), F32),
            V((DEV, SLOTS, ROWS), BF16), V((DEV, SLOTS, ROWS), BF16),
            V((DEV, SLOTS, 128), F32), V((DEV, SLOTS, 128), F32), V((ROWS, 2 * COLS), BF16),
            V((PARTS, DEV, SLOTS, WIDE), BF16), V((PARTS, DEV, SLOTS, WIDE), BF16),
            V((PARTS, DEV, SLOTS, WIDE), BF16), V((PARTS, DEV, SLOTS, WIDE), BF16),
            V((DEV, 1, 128), F32), V((DEV, 1, 128), F32),
            V((PARTS, ROWS, WIDE), F32), V((PARTS, ROWS, WIDE), F32), V((PARTS, 2, LEAF, WIDE), BF16),
            V((PARTS, ROWS, WIDE), F32), V((PARTS, ROWS, 2 * WIDE), BF16), V((PARTS, ROWS, WIDE), F32),
            V((ROWS, COLS), F32),
            V((PARTS, 4, 4, RANK, WIDE), BF16), V((PARTS, 4, 4, RANK, WIDE), BF16), V((32, RANK, WIDE), BF16),
            V((2, RANK, 16 * RANK), BF16), V((16 * RANK, WIDE), BF16),
            V((PARTS, 2, 4, RANK // 2, WIDE), BF16), V((PARTS, 2, 4, RANK // 2, WIDE), BF16),
            V((PARTS, 8, RANK, WIDE), BF16), V((8, 8, COLS), F32), V((16, 8, COLS), F32),
            dma((8,)), dma((PARTS,)), dma((PARTS, 16)), dma, dma((16,)), dma((PARTS,)), dma((PARTS, 16)),
            dma((PARTS, 4)), dma((PARTS, 4)), dma((PARTS, 4)), dma((PARTS, 4)), dma((PARTS,)), dma((PARTS,)),
            dma((2,)), dma((2,)), dma,
        ],
        compiler_params=pltpu.CompilerParams(
            collective_id=0, has_side_effects=True, vmem_limit_bytes=67_000_000
        ),
        name="dual_step",
    )(
        spread_owner.T, spread_row.T, spread_weight.T, near_list, far_list, top_block,
        basis, gram_term, near_block, leaf_basis, far_block, ascend, descend,
    )
    rows = ROWS // 4
    return tuple(
        pl.pallas_call(
            finish,
            grid=(4,),
            out_shape=(jax.ShapeDtypeStruct((ROWS, COLS), F32), jax.ShapeDtypeStruct((3, COLS), F32)),
            in_specs=[
                pl.BlockSpec((8, COLS), lambda i: (0, 0)),
                pl.BlockSpec((2, rows, COLS), lambda i: (0, i, 0)),
                pl.BlockSpec((rows, COLS), lambda i: (i, 0)),
            ],
            out_specs=(pl.BlockSpec((rows, COLS), lambda i: (i, 0)), pl.BlockSpec((3, COLS), lambda i: (0, 0))),
            name="finish",
        )(total, basis, image)
    )


def solution(mesh):
    finer = Mesh(mesh.devices.reshape(4, 4, 4, 2), AXES)
    split = P(BRANCH_GROUP)
    return jax.shard_map(
        body,
        mesh=finer,
        in_specs=(
            P(None, BRANCH_GROUP, None), split, split, split, split, split, split,
            split, split, split, split, split, P(GROUP, None),
        ),
        out_specs=(P(BRANCH_GROUP, None), P()),
        check_vma=False,
    )
```

```python
import jax
import jax.numpy as jnp
from jax import lax
from jax.experimental import pallas as pl
from jax.experimental.pallas import tpu as pltpu
from jax.sharding import Mesh
from jax.sharding import PartitionSpec as P

AXES = ("branch_0", "branch_1", "group_0", "group_1")
BRANCH_GROUP = AXES
GROUP = AXES[2:]
MESH = pl.DeviceIdType.MESH
F32 = jnp.float32
BF16 = jnp.bfloat16
DEV = 128
SLOTS = 32
ROWS = 1024
LEAF = 512
RANK = 64
COLS = 256
TOTAL = DEV * ROWS
SELF = 2
HELD = 12
PARTS = 2
WIDE = COLS // PARTS


def dot(a, b):
    return jnp.dot(a, b, preferred_element_type=F32)


def dot_t(a, b):
    return lax.dot_general(a, b, (((0,), (0,)), ((), ())), preferred_element_type=F32)


def kernel(
    owner_ref, row_ref, weight_ref, near_list, far_list, top_ref,
    basis_hbm, gram_hbm, near_hbm, base_hbm, far_hbm, asc_hbm, desc_hbm,
    image_hbm, total_ref,
    basis, gram, near, base, far, asc, desc,
    rank_of, rank_low, weight_of, row_of, count_of,
    pick, place, slot_weight, slot_low, vec,
    send, got, reply, back,
    row_send, row_got,
    acc, first, first_low, near_sum, dual_two, image, image_out,
    ag0, ag1, coeff, far_flat, far_in,
    par1, par2, tops, sums1, sums2,
    load_sem, send_sem, got_sem, row_send_sem, row_sem, reply_sem, back_sem,
    ag_send_sem, ag_sem, par_send_sem, par_sem, top_send_sem, top_sem, sum_send_sem, sum_sem, out_sem,
):
    z, x, y, c = (lax.axis_index(a) for a in AXES)
    zs = [z] + [lax.rem(z + d, 4) for d in (1, 2, 3)]
    xs = [x] + [lax.rem(x + d, 4) for d in (1, 2, 3)]
    ys = [y] + [lax.rem(y + d, 4) for d in (1, 2, 3)]
    cs = [c, 1 - c]
    branch = z * 4 + x
    group = y * 2 + c
    me = branch * 8 + group

    def remote(src, dst, send_s, recv_s, to):
        pltpu.make_async_remote_copy(
            src_ref=src, dst_ref=dst, send_sem=send_s, recv_sem=recv_s, device_id=to, device_id_type=MESH
        ).start()

    def wait_for(ref, sem):
        pltpu.make_async_copy(ref, ref, sem).wait()

    barrier = pltpu.get_barrier_semaphore()
    for k in range(1, DEV):
        pl.semaphore_signal(
            barrier, inc=1,
            device_id=(zs[k // 32], xs[k // 8 % 4], ys[k // 2 % 4], cs[k % 2]),
            device_id_type=MESH,
        )

    loads = [
        pltpu.make_async_copy(src, dst, load_sem.at[n])
        for n, (src, dst) in enumerate(
            (
                (basis_hbm.at[1], basis.at[1]), (basis_hbm.at[0], basis.at[0]), (gram_hbm, gram),
                (base_hbm, base), (asc_hbm, asc), (desc_hbm, desc), (far_hbm, far), (near_hbm, near),
            )
        )
    ]
    for load in loads:
        load.start()

    owners = lax.broadcasted_iota(jnp.int32, (DEV, ROWS), 0)
    hit0 = jnp.broadcast_to(owner_ref[0:1, :], (DEV, ROWS)) == owners
    hit1 = jnp.broadcast_to(owner_ref[1:2, :], (DEV, ROWS)) == owners
    hit = jnp.where(hit0, 1.0, 0.0) + jnp.where(hit1, 1.0, 0.0)
    weight_of[...] = jnp.where(
        hit0, jnp.broadcast_to(weight_ref[0:1, :], (DEV, ROWS)),
        jnp.broadcast_to(weight_ref[1:2, :], (DEV, ROWS)),
    )
    row_of[...] = jnp.where(
        hit0, jnp.broadcast_to(row_ref[0:1, :], (DEV, ROWS)),
        jnp.broadcast_to(row_ref[1:2, :], (DEV, ROWS)),
    ).astype(F32)
    upto = jnp.where(
        lax.broadcasted_iota(jnp.int32, (128, 128), 0) <= lax.broadcasted_iota(jnp.int32, (128, 128), 1),
        1.0, 0.0,
    ).astype(BF16)
    before = jnp.zeros((DEV, 1), F32)
    for n in range(ROWS // 128):
        part = hit[:, n * 128 : (n + 1) * 128]
        count = dot(part.astype(BF16), upto) + before
        rank_of[:, n * 128 : (n + 1) * 128] = jnp.where(part > 0.5, count - 1.0, -1.0)
        before = count[:, 127:128]
    count_of[...] = jnp.broadcast_to(before, (DEV, 128))
    rank_low[...] = jnp.where(rank_of[...] >= 0.0, rank_of[...] + jnp.broadcast_to(before, (DEV, ROWS)), -1.0)

    loads[0].wait()
    vector = basis[1]
    vec[:, 0:COLS] = vector.astype(BF16)
    vec[:, COLS:] = (vector - vector.astype(BF16).astype(F32)).astype(BF16)

    def offsets(i):
        return lax.rem(i + 2, 4), lax.rem(i + 2 + i // 4, 4)

    def to_group(i):
        dz, dx = offsets(i)
        return lax.rem(z + dz, 4), lax.rem(x + dx, 4)

    def from_group(i):
        dz, dx = offsets(i)
        return lax.rem(z + 4 - dz, 4), lax.rem(x + 4 - dx, 4)

    def spread_out(buf, into, s_sem, r_sem, i, tz, tx):
        mine = i * 8 + group
        for dy in (2, 1, 3, 0):
            for dc in (1, 0):
                src = buf.at[i * 8 + ys[dy] * 2 + cs[dc]]
                if dy == 0 and dc == 0:

                    @pl.when(i != SELF)
                    def _():
                        remote(src, into.at[mine], s_sem, r_sem.at[i], (tz, tx, ys[dy], cs[dc]))

                    @pl.when(i == SELF)
                    def _():
                        pltpu.make_async_copy(src, into.at[mine], r_sem.at[i]).start()
                else:
                    remote(src, into.at[mine], s_sem, r_sem.at[i], (tz, tx, ys[dy], cs[dc]))

    slot_at = lax.broadcasted_iota(jnp.int32, (SLOTS, ROWS), 0).astype(F32)
    slot_col = lax.broadcasted_iota(jnp.int32, (SLOTS, COLS), 0).astype(F32)
    lane_at = lax.broadcasted_iota(jnp.int32, (SLOTS, 128), 1)

    def fill(i, carry):
        tz, tx = to_group(i)
        eight = pl.ds(pl.multiple_of((tz * 4 + tx) * 8, 8), 8)
        ranks, lows, weights, rows = rank_of[eight, :], rank_low[eight, :], weight_of[eight, :], row_of[eight, :]
        counts = count_of[eight, :]
        listed = jnp.zeros((SLOTS, 128), F32)
        scales = []
        for o in range(8):
            mask = (jnp.broadcast_to(ranks[o : o + 1, :], (SLOTS, ROWS)) == slot_at) | (
                jnp.broadcast_to(lows[o : o + 1, :], (SLOTS, ROWS)) == slot_at
            )
            pick[i * 8 + o] = jnp.where(mask, 1.0, 0.0).astype(BF16)
            scale = jnp.sum(
                jnp.where(mask, jnp.broadcast_to(weights[o : o + 1, :], (SLOTS, ROWS)), 0.0), axis=1, keepdims=True
            )
            row = jnp.sum(
                jnp.where(mask, jnp.broadcast_to(rows[o : o + 1, :], (SLOTS, ROWS)), 0.0), axis=1, keepdims=True
            )
            row = jnp.broadcast_to(row, (SLOTS, 128)) + jnp.where(
                slot_col[:, 0:128] >= jnp.broadcast_to(counts[o : o + 1, :], (SLOTS, 128)), float(ROWS), 0.0
            )
            listed = jnp.where(lane_at == o, row, listed)
            slot_weight[i * 8 + o] = jnp.broadcast_to(scale, (SLOTS, 128))
            scales.append(jnp.broadcast_to(scale, (SLOTS, COLS)))
        turned = jnp.transpose(listed)
        for o in range(8):
            row_send[i * 8 + o, :, 0:SLOTS] = turned[o : o + 1, :]

        values = dot(pick[pl.ds(i * 8, 8)].reshape(8 * SLOTS, ROWS), vec[...])
        for o in range(8):
            part = values[o * SLOTS : (o + 1) * SLOTS, :]
            part = (part[:, 0:COLS] + part[:, COLS:]) * scales[o]
            high = part.astype(BF16).astype(F32)
            count = jnp.broadcast_to(counts[o : o + 1, 0:1], (SLOTS, COLS))
            sent = jnp.where(slot_col >= count, part - high, high).astype(BF16)
            for p in range(PARTS):
                send[p, i * 8 + o] = sent[:, p * WIDE : (p + 1) * WIDE]

        @pl.when(i == 0)
        def _():
            pl.semaphore_wait(barrier, DEV - 1)

        spread_out(row_send, row_got, row_send_sem, row_sem, i, tz, tx)
        spread_out(send.at[0], got.at[0], send_sem.at[0], got_sem.at[0], i, tz, tx)
        return carry

    lax.fori_loop(0, 16, fill, 0)

    def fill_rest(i, carry):
        spread_out(send.at[1], got.at[1], send_sem.at[1], got_sem.at[1], i, *to_group(i))
        return carry

    for n in range(2, 8):
        loads[n].wait()
    acc[...] = jnp.zeros_like(acc)
    image[...] = jnp.zeros_like(image)
    row_at = lax.broadcasted_iota(jnp.int32, (SLOTS, ROWS), 1).astype(F32)

    def find_places(i, carry):
        wait_for(row_got.at[pl.ds(0, 8)], row_sem.at[i])
        turned = jnp.transpose(jnp.concatenate([row_got[i * 8 + o] for o in range(8)], axis=0))
        for o in range(8):
            row = turned[0:SLOTS, o : o + 1]
            low = row >= float(ROWS)
            slot_low[i * 8 + o] = jnp.broadcast_to(jnp.where(low, 1.0, 0.0), (SLOTS, 128))
            row = jnp.where(low, row - float(ROWS), row)
            place[i * 8 + o] = jnp.where(jnp.broadcast_to(row, (SLOTS, ROWS)) == row_at, 1.0, 0.0).astype(BF16)
        return carry

    def four(q):
        return pl.ds(pl.multiple_of(q * 32, 32), 32)

    def gather(p, start, stop):
        def step(q, carry):
            for n in range(4):
                wait_for(got.at[p, pl.ds(0, 8)], got_sem.at[p, q * 4 + n])
            chosen = place[four(q)].reshape(32 * SLOTS, ROWS)
            acc[p] += dot_t(chosen, got[p, four(q)].reshape(32 * SLOTS, WIDE))
            return carry

        lax.fori_loop(start // 4, stop // 4, step, 0)

    half = RANK // 2

    def early(p):
        partial = jnp.zeros((RANK, WIDE), F32)
        for leaf, (slots, i, j) in enumerate(((ag0, z, x), (ag1, x, z))):
            rows = pl.ds(leaf * LEAF, LEAF)
            dual = acc[p, rows, :]
            passed = dual + dot_t(gram[leaf], dual.astype(BF16))
            first[p, rows, :] = passed
            first_low[p, leaf] = passed.astype(BF16)
            low = dot(base[leaf], first_low[p, leaf]).astype(BF16)
            slots[p, i, j] = low
            partial = partial + dot(asc[leaf], low)
        par1[p, 0, x] = partial[0:half].astype(BF16)
        par1[p, 1, z] = partial[half:].astype(BF16)
        for d in (1, 3, 2):
            remote(par1.at[p, 0, x], par1.at[p, 0, x], par_send_sem.at[p, 0], par_sem.at[p, 0], (z, xs[d], y, c))
            remote(par1.at[p, 1, z], par1.at[p, 1, z], par_send_sem.at[p, 1], par_sem.at[p, 1], (zs[d], x, y, c))
        for d in (1, 3, 2):
            remote(ag0.at[p, z, x], ag0.at[p, z, x], ag_send_sem.at[p, 0], ag_sem.at[p, 0], (z, xs[d], y, c))
            remote(ag1.at[p, x, z], ag1.at[p, x, z], ag_send_sem.at[p, 1], ag_sem.at[p, 1], (zs[d], x, y, c))

    def near_of(p, leaf):
        found = dot(near[leaf, 0], first_low[p, near_list[leaf, 0]])
        for k in range(1, 8):
            found = found + dot(near[leaf, k], first_low[p, near_list[leaf, k]])
        near_sum[p, pl.ds(leaf * LEAF, LEAF), :] = found

    three = pl.ds(0, 3)

    def summed(ref):
        return ((ref[0].astype(F32) + ref[1].astype(F32)) + (ref[2].astype(F32) + ref[3].astype(F32))).astype(BF16)

    def mid_a(p):
        wait_for(par1.at[p, 0, three], par_sem.at[p, 0])
        wait_for(par1.at[p, 1, three], par_sem.at[p, 1])
        par2[p, 0, z] = summed(par1.at[p, 0])
        par2[p, 1, x] = summed(par1.at[p, 1])
        for d in (1, 3, 2):
            remote(par2.at[p, 0, z], par2.at[p, 0, z], par_send_sem.at[p, 2], par_sem.at[p, 2], (zs[d], x, y, c))
            remote(par2.at[p, 1, x], par2.at[p, 1, x], par_send_sem.at[p, 3], par_sem.at[p, 3], (z, xs[d], y, c))
        wait_for(ag0.at[p, 0, three], ag_sem.at[p, 0])
        wait_for(ag1.at[p, 0, three], ag_sem.at[p, 1])
        for d in (1, 3, 2):
            remote(ag0.at[p, z], ag0.at[p, z], ag_send_sem.at[p, 2], ag_sem.at[p, 2], (zs[d], x, y, c))
            remote(ag1.at[p, x], ag1.at[p, x], ag_send_sem.at[p, 3], ag_sem.at[p, 3], (z, xs[d], y, c))

    def mid_b(p):
        wait_for(par2.at[p, 0, three], par_sem.at[p, 2])
        wait_for(par2.at[p, 1, three], par_sem.at[p, 3])
        tops[p, group, 0:half] = summed(par2.at[p, 0])
        tops[p, group, half:] = summed(par2.at[p, 1])
        for k in range(1, 8):
            remote(tops.at[p, group], tops.at[p, group], top_send_sem.at[p], top_sem.at[p], (z, x, ys[k // 2], cs[k % 2]))

    def mid_c(p):
        wait_for(tops.at[p, pl.ds(0, 7)], top_sem.at[p])
        field = dot(top_ref[...], tops[p].reshape(8 * RANK, WIDE)).astype(BF16)
        wait_for(ag0.at[p, three], ag_sem.at[p, 2])
        wait_for(ag1.at[p, three], ag_sem.at[p, 3])
        for b in range(16):
            coeff[2 * b] = ag0[p, b // 4, b % 4]
            coeff[2 * b + 1] = ag1[p, b % 4, b // 4]
        for leaf in range(2):
            for k in range(16):
                far_in[k * RANK : (k + 1) * RANK, :] = coeff[far_list[leaf, k]]
            rows = pl.ds(leaf * LEAF, LEAF)
            descent = (dot(far_flat[leaf], far_in[...]) + dot(desc[leaf], field)).astype(BF16)
            dual = first[p, rows, :] + near_sum[p, rows, :] + dot_t(base[leaf], descent)
            dual = dual + dot(gram[leaf], dual.astype(BF16))
            dual_two[p, rows, 0:WIDE] = dual.astype(BF16)
            dual_two[p, rows, WIDE:] = (dual - dual.astype(BF16).astype(F32)).astype(BF16)

    def answer(p, start, stop):
        def step(q, carry):
            both = dot(place[four(q)].reshape(32 * SLOTS, ROWS), dual_two[p])
            low = slot_low[four(q)].reshape(32 * SLOTS, 128) > 0.5
            reply[p, four(q)] = jnp.where(low, both[:, WIDE:], both[:, 0:WIDE]).astype(BF16).reshape(32, SLOTS, WIDE)
            for n in range(4):
                i = q * 4 + n
                spread_out(reply.at[p], back.at[p], reply_sem.at[p], back_sem.at[p], i, *from_group(i))
            return carry

        lax.fori_loop(start // 4, stop // 4, step, 0)

    def collect(p):
        def step(q, carry):
            for n in range(4):
                wait_for(back.at[p, pl.ds(0, 8)], back_sem.at[p, q * 4 + n])
            values = back[p, four(q)].reshape(32 * SLOTS, WIDE).astype(F32) * slot_weight[four(q)].reshape(32 * SLOTS, 128)
            high = values.astype(BF16)
            two = jnp.concatenate([high, (values - high.astype(F32)).astype(BF16)], axis=1)
            both = dot_t(pick[four(q)].reshape(32 * SLOTS, ROWS), two)
            image[p] += both[:, 0:WIDE] + both[:, WIDE:]
            return carry

        lax.fori_loop(0, 4, step, 0)

    def flatten_far():
        for leaf in range(2):
            for k in range(8):
                far_flat[leaf, :, k * 128 : (k + 1) * 128] = jnp.concatenate(
                    [far[leaf, 2 * k], far[leaf, 2 * k + 1]], axis=1
                )

    lax.fori_loop(0, HELD, fill_rest, 0)
    lax.fori_loop(0, 16, find_places, 0)
    flatten_far()
    gather(0, 0, 16)
    early(0)
    lax.fori_loop(HELD, 16, fill_rest, 0)
    near_of(0, 0)
    near_of(0, 1)
    gather(1, 0, 8)
    mid_a(0)
    gather(1, 8, 16)
    early(1)
    mid_b(0)
    near_of(1, 0)
    mid_a(1)
    mid_c(0)
    answer(0, 0, 8)
    mid_b(1)
    answer(0, 8, 16)
    near_of(1, 1)
    mid_c(1)
    answer(1, 0, 16)
    loads[1].wait()
    v0, v1 = basis[0], basis[1]
    mutual = [jnp.sum(a * b, axis=0, keepdims=True) for a, b in ((v0, v0), (v0, v1), (v1, v1))]
    collect(0)
    collect(1)

    found = jnp.concatenate([image[0], image[1]], axis=1)
    image_out[...] = found
    cross = [jnp.sum(basis[k] * found, axis=0, keepdims=True) for k in range(2)]
    whole = jnp.sum(found * found, axis=0, keepdims=True)
    sums1[group] = jnp.concatenate(cross + [whole] + mutual + [jnp.zeros((2, COLS), F32)], axis=0)
    for k in range(1, 8):
        remote(sums1.at[group], sums1.at[group], sum_send_sem.at[0], sum_sem.at[0], (z, x, ys[k // 2], cs[k % 2]))
    leave = pltpu.make_async_copy(image_out, image_hbm, out_sem)
    leave.start()
    wait_for(sums1.at[pl.ds(0, 7)], sum_sem.at[0])
    sums2[branch] = jnp.sum(sums1[...], axis=0)
    for k in range(1, 16):
        remote(sums2.at[branch], sums2.at[branch], sum_send_sem.at[1], sum_sem.at[1], (zs[k // 4], xs[k % 4], y, c))
    wait_for(row_send.at[pl.ds(0, DEV - 1)], row_send_sem)
    for p in range(PARTS):
        wait_for(send.at[p, pl.ds(0, DEV - 1)], send_sem.at[p])
        wait_for(reply.at[p, pl.ds(0, DEV - 1)], reply_sem.at[p])
        wait_for(ag0.at[p, 0, three], ag_send_sem.at[p, 0])
        wait_for(ag1.at[p, 0, three], ag_send_sem.at[p, 1])
        wait_for(ag0.at[p, three], ag_send_sem.at[p, 2])
        wait_for(ag1.at[p, three], ag_send_sem.at[p, 3])
        for n in range(4):
            wait_for(par1.at[p, 0, three], par_send_sem.at[p, n])
        wait_for(tops.at[p, pl.ds(0, 7)], top_send_sem.at[p])
    leave.wait()
    wait_for(sums1.at[pl.ds(0, 7)], sum_send_sem.at[0])
    wait_for(sums2.at[pl.ds(0, 15)], sum_sem.at[1])
    wait_for(sums2.at[pl.ds(0, 15)], sum_send_sem.at[1])
    total = jnp.sum(sums2[...], axis=0) * (1.0 / TOTAL)
    p0, p1, sq = total[0:1], total[1:2], total[2:3]
    m00, m01, m11 = total[3:4], total[4:5], total[5:6]
    square = sq - 2.0 * (p0 * p0 + p1 * p1) + (p0 * p0 * m00 + 2.0 * (p0 * p1) * m01 + p1 * p1 * m11)
    norm = jnp.sqrt(square + 1e-6)
    total_ref[...] = jnp.concatenate([p0, p1, norm, 1.0 / norm, jnp.zeros((4, COLS), F32)], axis=0)


def finish(total_ref, basis_ref, image_ref, out_ref, hess_ref):
    p0, p1, scale = total_ref[0:1], total_ref[1:2], total_ref[3:4]
    out_ref[...] = (image_ref[...] - (p0 * basis_ref[0] + p1 * basis_ref[1])) * scale
    hess_ref[...] = total_ref[0:3]


def body(
    basis, spread_owner, spread_row, spread_weight, gram_term, near_block, near_list,
    leaf_basis, far_block, far_list, ascend, descend, top_block,
):
    vmem = pl.BlockSpec(memory_space=pltpu.VMEM)
    smem = pl.BlockSpec(memory_space=pltpu.SMEM)
    hbm = pl.BlockSpec(memory_space=pl.ANY)
    dma = pltpu.SemaphoreType.DMA
    V = pltpu.VMEM
    image, total = pl.pallas_call(
        kernel,
        out_shape=(
            jax.ShapeDtypeStruct((ROWS, COLS), F32),
            jax.ShapeDtypeStruct((8, COLS), F32),
        ),
        in_specs=[vmem] * 3 + [smem] * 2 + [vmem] + [hbm] * 7,
        out_specs=(hbm, vmem),
        scratch_shapes=[
            V((2, ROWS, COLS), F32), V((2, LEAF, LEAF), BF16), V((2, 8, LEAF, LEAF), BF16),
            V((2, RANK, LEAF), BF16), V((2, 16, RANK, RANK), BF16), V((2, RANK, RANK), BF16),
            V((2, RANK, RANK), BF16),
            V((DEV, ROWS), F32), V((DEV, ROWS), F32), V((DEV, ROWS), F32), V((DEV, ROWS), F32), V((DEV, 128), F32),
            V((DEV, SLOTS, ROWS), BF16), V((DEV, SLOTS, ROWS), BF16),
            V((DEV, SLOTS, 128), F32), V((DEV, SLOTS, 128), F32), V((ROWS, 2 * COLS), BF16),
            V((PARTS, DEV, SLOTS, WIDE), BF16), V((PARTS, DEV, SLOTS, WIDE), BF16),
            V((PARTS, DEV, SLOTS, WIDE), BF16), V((PARTS, DEV, SLOTS, WIDE), BF16),
            V((DEV, 1, 128), F32), V((DEV, 1, 128), F32),
            V((PARTS, ROWS, WIDE), F32), V((PARTS, ROWS, WIDE), F32), V((PARTS, 2, LEAF, WIDE), BF16),
            V((PARTS, ROWS, WIDE), F32), V((PARTS, ROWS, 2 * WIDE), BF16), V((PARTS, ROWS, WIDE), F32),
            V((ROWS, COLS), F32),
            V((PARTS, 4, 4, RANK, WIDE), BF16), V((PARTS, 4, 4, RANK, WIDE), BF16), V((32, RANK, WIDE), BF16),
            V((2, RANK, 16 * RANK), BF16), V((16 * RANK, WIDE), BF16),
            V((PARTS, 2, 4, RANK // 2, WIDE), BF16), V((PARTS, 2, 4, RANK // 2, WIDE), BF16),
            V((PARTS, 8, RANK, WIDE), BF16), V((8, 8, COLS), F32), V((16, 8, COLS), F32),
            dma((8,)), dma((PARTS,)), dma((PARTS, 16)), dma, dma((16,)), dma((PARTS,)), dma((PARTS, 16)),
            dma((PARTS, 4)), dma((PARTS, 4)), dma((PARTS, 4)), dma((PARTS, 4)), dma((PARTS,)), dma((PARTS,)),
            dma((2,)), dma((2,)), dma,
        ],
        compiler_params=pltpu.CompilerParams(
            collective_id=0, has_side_effects=True, vmem_limit_bytes=67_000_000
        ),
        name="dual_step",
    )(
        spread_owner.T, spread_row.T, spread_weight.T, near_list, far_list, top_block,
        basis, gram_term, near_block, leaf_basis, far_block, ascend, descend,
    )
    rows = ROWS // 4
    return tuple(
        pl.pallas_call(
            finish,
            grid=(4,),
            out_shape=(jax.ShapeDtypeStruct((ROWS, COLS), F32), jax.ShapeDtypeStruct((3, COLS), F32)),
            in_specs=[
                pl.BlockSpec((8, COLS), lambda i: (0, 0)),
                pl.BlockSpec((2, rows, COLS), lambda i: (0, i, 0)),
                pl.BlockSpec((rows, COLS), lambda i: (i, 0)),
            ],
            out_specs=(pl.BlockSpec((rows, COLS), lambda i: (i, 0)), pl.BlockSpec((3, COLS), lambda i: (0, 0))),
            name="finish",
        )(total, basis, image)
    )


def solution(mesh):
    finer = Mesh(mesh.devices.reshape(4, 4, 4, 2), AXES)
    split = P(BRANCH_GROUP)
    return jax.shard_map(
        body,
        mesh=finer,
        in_specs=(
            P(None, BRANCH_GROUP, None), split, split, split, split, split, split,
            split, split, split, split, split, P(GROUP, None),
        ),
        out_specs=(P(BRANCH_GROUP, None), P()),
        check_vma=False,
    )
```

```python
import jax
import jax.numpy as jnp
from jax import lax
from jax.experimental import pallas as pl
from jax.experimental.pallas import tpu as pltpu
from jax.sharding import Mesh
from jax.sharding import PartitionSpec as P

AXES = ("branch_0", "branch_1", "group_0", "group_1")
BRANCH_GROUP = AXES
GROUP = AXES[2:]
MESH = pl.DeviceIdType.MESH
F32 = jnp.float32
BF16 = jnp.bfloat16
DEV = 128
SLOTS = 32
ROWS = 1024
LEAF = 512
RANK = 64
COLS = 256
TOTAL = DEV * ROWS
SELF = 2
LIMIT_A = 57_000_000
LIMIT_B = 4_000_000
STEP = 128
HELD = 12
PARTS = 2
WIDE = COLS // PARTS


def dot(a, b):
    return jnp.dot(a, b, preferred_element_type=F32)


def dot_t(a, b):
    return lax.dot_general(a, b, (((0,), (0,)), ((), ())), preferred_element_type=F32)


def kernel(
    owner_ref, row_ref, weight_ref, near_list, far_list, top_ref,
    basis_hbm, gram_hbm, near_hbm, base_hbm, far_hbm, asc_hbm, desc_hbm,
    image_hbm, total_ref,
    basis, gram, near, base, far, asc, desc,
    rank_of, rank_low, weight_of, row_of, count_of,
    pick, place, slot_weight, slot_low, vec,
    send, got, reply, back,
    row_send, row_got,
    acc, first, first_low, near_sum, dual_two, image,
    ag0, ag1, coeff, far_flat, far_in,
    par1, par2, tops, sums1, sums2,
    load_sem, send_sem, got_sem, row_send_sem, row_sem, reply_sem, back_sem,
    ag_send_sem, ag_sem, par_send_sem, par_sem, top_send_sem, top_sem, sum_send_sem, sum_sem, out_sem,
):
    z, x, y, c = (lax.axis_index(a) for a in AXES)
    zs = [z] + [lax.rem(z + d, 4) for d in (1, 2, 3)]
    xs = [x] + [lax.rem(x + d, 4) for d in (1, 2, 3)]
    ys = [y] + [lax.rem(y + d, 4) for d in (1, 2, 3)]
    cs = [c, 1 - c]
    branch = z * 4 + x
    group = y * 2 + c
    me = branch * 8 + group

    def remote(src, dst, send_s, recv_s, to):
        pltpu.make_async_remote_copy(
            src_ref=src, dst_ref=dst, send_sem=send_s, recv_sem=recv_s, device_id=to, device_id_type=MESH
        ).start()

    def wait_for(ref, sem):
        pltpu.make_async_copy(ref, ref, sem).wait()

    barrier = pltpu.get_barrier_semaphore()
    for k in range(1, DEV):
        pl.semaphore_signal(
            barrier, inc=1,
            device_id=(zs[k // 32], xs[k // 8 % 4], ys[k // 2 % 4], cs[k % 2]),
            device_id_type=MESH,
        )

    loads = [
        pltpu.make_async_copy(src, dst, load_sem.at[n])
        for n, (src, dst) in enumerate(
            (
                (basis_hbm.at[1], basis.at[1]), (basis_hbm.at[0], basis.at[0]), (gram_hbm, gram),
                (base_hbm, base), (asc_hbm, asc), (desc_hbm, desc), (far_hbm, far), (near_hbm, near),
            )
        )
    ]
    for load in loads:
        load.start()

    owners = lax.broadcasted_iota(jnp.int32, (DEV, ROWS), 0)
    hit0 = jnp.broadcast_to(owner_ref[0:1, :], (DEV, ROWS)) == owners
    hit1 = jnp.broadcast_to(owner_ref[1:2, :], (DEV, ROWS)) == owners
    hit = jnp.where(hit0, 1.0, 0.0) + jnp.where(hit1, 1.0, 0.0)
    weight_of[...] = jnp.where(
        hit0, jnp.broadcast_to(weight_ref[0:1, :], (DEV, ROWS)),
        jnp.broadcast_to(weight_ref[1:2, :], (DEV, ROWS)),
    )
    row_of[...] = jnp.where(
        hit0, jnp.broadcast_to(row_ref[0:1, :], (DEV, ROWS)),
        jnp.broadcast_to(row_ref[1:2, :], (DEV, ROWS)),
    ).astype(F32)
    upto = jnp.where(
        lax.broadcasted_iota(jnp.int32, (128, 128), 0) <= lax.broadcasted_iota(jnp.int32, (128, 128), 1),
        1.0, 0.0,
    ).astype(BF16)
    before = jnp.zeros((DEV, 1), F32)
    for n in range(ROWS // 128):
        part = hit[:, n * 128 : (n + 1) * 128]
        count = dot(part.astype(BF16), upto) + before
        rank_of[:, n * 128 : (n + 1) * 128] = jnp.where(part > 0.5, count - 1.0, -1.0)
        before = count[:, 127:128]
    count_of[...] = jnp.broadcast_to(before, (DEV, 128))
    rank_low[...] = jnp.where(rank_of[...] >= 0.0, rank_of[...] + jnp.broadcast_to(before, (DEV, ROWS)), -1.0)

    loads[0].wait()
    vector = basis[1]
    vec[:, 0:COLS] = vector.astype(BF16)
    vec[:, COLS:] = (vector - vector.astype(BF16).astype(F32)).astype(BF16)

    def offsets(i):
        return lax.rem(i + 2, 4), lax.rem(i + 2 + i // 4, 4)

    def to_group(i):
        dz, dx = offsets(i)
        return lax.rem(z + dz, 4), lax.rem(x + dx, 4)

    def from_group(i):
        dz, dx = offsets(i)
        return lax.rem(z + 4 - dz, 4), lax.rem(x + 4 - dx, 4)

    def spread_out(buf, into, s_sem, r_sem, i, tz, tx):
        mine = i * 8 + group
        for dy in (2, 1, 3, 0):
            for dc in (1, 0):
                src = buf.at[i * 8 + ys[dy] * 2 + cs[dc]]
                if dy == 0 and dc == 0:

                    @pl.when(i != SELF)
                    def _():
                        remote(src, into.at[mine], s_sem, r_sem.at[i], (tz, tx, ys[dy], cs[dc]))

                    @pl.when(i == SELF)
                    def _():
                        pltpu.make_async_copy(src, into.at[mine], r_sem.at[i]).start()
                else:
                    remote(src, into.at[mine], s_sem, r_sem.at[i], (tz, tx, ys[dy], cs[dc]))

    slot_at = lax.broadcasted_iota(jnp.int32, (SLOTS, ROWS), 0).astype(F32)
    slot_col = lax.broadcasted_iota(jnp.int32, (SLOTS, COLS), 0).astype(F32)
    lane_at = lax.broadcasted_iota(jnp.int32, (SLOTS, 128), 1)

    def fill(i, carry):
        tz, tx = to_group(i)
        eight = pl.ds(pl.multiple_of((tz * 4 + tx) * 8, 8), 8)
        ranks, lows, weights, rows = rank_of[eight, :], rank_low[eight, :], weight_of[eight, :], row_of[eight, :]
        counts = count_of[eight, :]
        listed = jnp.zeros((SLOTS, 128), F32)
        scales = []
        for o in range(8):
            mask = (jnp.broadcast_to(ranks[o : o + 1, :], (SLOTS, ROWS)) == slot_at) | (
                jnp.broadcast_to(lows[o : o + 1, :], (SLOTS, ROWS)) == slot_at
            )
            pick[i * 8 + o] = jnp.where(mask, 1.0, 0.0).astype(BF16)
            scale = jnp.sum(
                jnp.where(mask, jnp.broadcast_to(weights[o : o + 1, :], (SLOTS, ROWS)), 0.0), axis=1, keepdims=True
            )
            row = jnp.sum(
                jnp.where(mask, jnp.broadcast_to(rows[o : o + 1, :], (SLOTS, ROWS)), 0.0), axis=1, keepdims=True
            )
            row = jnp.broadcast_to(row, (SLOTS, 128)) + jnp.where(
                slot_col[:, 0:128] >= jnp.broadcast_to(counts[o : o + 1, :], (SLOTS, 128)), float(ROWS), 0.0
            )
            listed = jnp.where(lane_at == o, row, listed)
            slot_weight[i * 8 + o] = jnp.broadcast_to(scale, (SLOTS, 128))
            scales.append(jnp.broadcast_to(scale, (SLOTS, COLS)))
        turned = jnp.transpose(listed)
        for o in range(8):
            row_send[i * 8 + o, :, 0:SLOTS] = turned[o : o + 1, :]

        values = dot(pick[pl.ds(i * 8, 8)].reshape(8 * SLOTS, ROWS), vec[...])
        for o in range(8):
            part = values[o * SLOTS : (o + 1) * SLOTS, :]
            part = (part[:, 0:COLS] + part[:, COLS:]) * scales[o]
            high = part.astype(BF16).astype(F32)
            count = jnp.broadcast_to(counts[o : o + 1, 0:1], (SLOTS, COLS))
            sent = jnp.where(slot_col >= count, part - high, high).astype(BF16)
            for p in range(PARTS):
                send[p, i * 8 + o] = sent[:, p * WIDE : (p + 1) * WIDE]

        @pl.when(i == 0)
        def _():
            pl.semaphore_wait(barrier, DEV - 1)

        spread_out(row_send, row_got, row_send_sem, row_sem, i, tz, tx)
        spread_out(send.at[0], got.at[0], send_sem.at[0], got_sem.at[0], i, tz, tx)
        return carry

    lax.fori_loop(0, 16, fill, 0)

    def fill_rest(i, carry):
        spread_out(send.at[1], got.at[1], send_sem.at[1], got_sem.at[1], i, *to_group(i))
        return carry

    for n in range(2, 8):
        loads[n].wait()
    acc[...] = jnp.zeros_like(acc)
    image[...] = jnp.zeros_like(image)
    row_at = lax.broadcasted_iota(jnp.int32, (SLOTS, ROWS), 1).astype(F32)

    def find_places(i, carry):
        wait_for(row_got.at[pl.ds(0, 8)], row_sem.at[i])
        turned = jnp.transpose(jnp.concatenate([row_got[i * 8 + o] for o in range(8)], axis=0))
        for o in range(8):
            row = turned[0:SLOTS, o : o + 1]
            low = row >= float(ROWS)
            slot_low[i * 8 + o] = jnp.broadcast_to(jnp.where(low, 1.0, 0.0), (SLOTS, 128))
            row = jnp.where(low, row - float(ROWS), row)
            place[i * 8 + o] = jnp.where(jnp.broadcast_to(row, (SLOTS, ROWS)) == row_at, 1.0, 0.0).astype(BF16)
        return carry

    def four(q):
        return pl.ds(pl.multiple_of(q * 32, 32), 32)

    def gather(p, start, stop):
        def step(q, carry):
            for n in range(4):
                wait_for(got.at[p, pl.ds(0, 8)], got_sem.at[p, q * 4 + n])
            chosen = place[four(q)].reshape(32 * SLOTS, ROWS)
            acc[p] += dot_t(chosen, got[p, four(q)].reshape(32 * SLOTS, WIDE))
            return carry

        lax.fori_loop(start // 4, stop // 4, step, 0)

    half = RANK // 2

    def early(p):
        partial = jnp.zeros((RANK, WIDE), F32)
        for leaf, (slots, i, j) in enumerate(((ag0, z, x), (ag1, x, z))):
            rows = pl.ds(leaf * LEAF, LEAF)
            dual = acc[p, rows, :]
            passed = dual + dot_t(gram[leaf], dual.astype(BF16))
            first[p, rows, :] = passed
            first_low[p, leaf] = passed.astype(BF16)
            low = dot(base[leaf], first_low[p, leaf]).astype(BF16)
            slots[p, i, j] = low
            partial = partial + dot(asc[leaf], low)
        par1[p, 0, x] = partial[0:half].astype(BF16)
        par1[p, 1, z] = partial[half:].astype(BF16)
        for d in (1, 3, 2):
            remote(par1.at[p, 0, x], par1.at[p, 0, x], par_send_sem.at[p, 0], par_sem.at[p, 0], (z, xs[d], y, c))
            remote(par1.at[p, 1, z], par1.at[p, 1, z], par_send_sem.at[p, 1], par_sem.at[p, 1], (zs[d], x, y, c))
        for d in (1, 3, 2):
            remote(ag0.at[p, z, x], ag0.at[p, z, x], ag_send_sem.at[p, 0], ag_sem.at[p, 0], (z, xs[d], y, c))
            remote(ag1.at[p, x, z], ag1.at[p, x, z], ag_send_sem.at[p, 1], ag_sem.at[p, 1], (zs[d], x, y, c))

    def near_of(p, leaf):
        found = dot(near[leaf, 0], first_low[p, near_list[leaf, 0]])
        for k in range(1, 8):
            found = found + dot(near[leaf, k], first_low[p, near_list[leaf, k]])
        near_sum[p, pl.ds(leaf * LEAF, LEAF), :] = found

    three = pl.ds(0, 3)

    def summed(ref):
        return ((ref[0].astype(F32) + ref[1].astype(F32)) + (ref[2].astype(F32) + ref[3].astype(F32))).astype(BF16)

    def mid_a(p):
        wait_for(par1.at[p, 0, three], par_sem.at[p, 0])
        wait_for(par1.at[p, 1, three], par_sem.at[p, 1])
        par2[p, 0, z] = summed(par1.at[p, 0])
        par2[p, 1, x] = summed(par1.at[p, 1])
        for d in (1, 3, 2):
            remote(par2.at[p, 0, z], par2.at[p, 0, z], par_send_sem.at[p, 2], par_sem.at[p, 2], (zs[d], x, y, c))
            remote(par2.at[p, 1, x], par2.at[p, 1, x], par_send_sem.at[p, 3], par_sem.at[p, 3], (z, xs[d], y, c))
        wait_for(ag0.at[p, 0, three], ag_sem.at[p, 0])
        wait_for(ag1.at[p, 0, three], ag_sem.at[p, 1])
        for d in (1, 3, 2):
            remote(ag0.at[p, z], ag0.at[p, z], ag_send_sem.at[p, 2], ag_sem.at[p, 2], (zs[d], x, y, c))
            remote(ag1.at[p, x], ag1.at[p, x], ag_send_sem.at[p, 3], ag_sem.at[p, 3], (z, xs[d], y, c))

    def mid_b(p):
        wait_for(par2.at[p, 0, three], par_sem.at[p, 2])
        wait_for(par2.at[p, 1, three], par_sem.at[p, 3])
        tops[p, group, 0:half] = summed(par2.at[p, 0])
        tops[p, group, half:] = summed(par2.at[p, 1])
        for k in range(1, 8):
            remote(tops.at[p, group], tops.at[p, group], top_send_sem.at[p], top_sem.at[p], (z, x, ys[k // 2], cs[k % 2]))

    def mid_c(p):
        wait_for(tops.at[p, pl.ds(0, 7)], top_sem.at[p])
        field = dot(top_ref[...], tops[p].reshape(8 * RANK, WIDE)).astype(BF16)
        wait_for(ag0.at[p, three], ag_sem.at[p, 2])
        wait_for(ag1.at[p, three], ag_sem.at[p, 3])
        for b in range(16):
            coeff[2 * b] = ag0[p, b // 4, b % 4]
            coeff[2 * b + 1] = ag1[p, b % 4, b // 4]
        for leaf in range(2):
            for k in range(16):
                far_in[k * RANK : (k + 1) * RANK, :] = coeff[far_list[leaf, k]]
            rows = pl.ds(leaf * LEAF, LEAF)
            descent = (dot(far_flat[leaf], far_in[...]) + dot(desc[leaf], field)).astype(BF16)
            dual = first[p, rows, :] + near_sum[p, rows, :] + dot_t(base[leaf], descent)
            dual = dual + dot(gram[leaf], dual.astype(BF16))
            dual_two[p, rows, 0:WIDE] = dual.astype(BF16)
            dual_two[p, rows, WIDE:] = (dual - dual.astype(BF16).astype(F32)).astype(BF16)

    def answer(p, start, stop):
        def step(q, carry):
            both = dot(place[four(q)].reshape(32 * SLOTS, ROWS), dual_two[p])
            low = slot_low[four(q)].reshape(32 * SLOTS, 128) > 0.5
            reply[p, four(q)] = jnp.where(low, both[:, WIDE:], both[:, 0:WIDE]).astype(BF16).reshape(32, SLOTS, WIDE)
            for n in range(4):
                i = q * 4 + n
                spread_out(reply.at[p], back.at[p], reply_sem.at[p], back_sem.at[p], i, *from_group(i))
            return carry

        lax.fori_loop(start // 4, stop // 4, step, 0)

    def collect(p):
        def step(q, carry):
            for n in range(4):
                wait_for(back.at[p, pl.ds(0, 8)], back_sem.at[p, q * 4 + n])
            values = back[p, four(q)].reshape(32 * SLOTS, WIDE).astype(F32) * slot_weight[four(q)].reshape(32 * SLOTS, 128)
            high = values.astype(BF16)
            two = jnp.concatenate([high, (values - high.astype(F32)).astype(BF16)], axis=1)
            both = dot_t(pick[four(q)].reshape(32 * SLOTS, ROWS), two)
            image[p] += both[:, 0:WIDE] + both[:, WIDE:]
            return carry

        lax.fori_loop(0, 4, step, 0)

    def flatten_far():
        for leaf in range(2):
            for k in range(8):
                far_flat[leaf, :, k * 128 : (k + 1) * 128] = jnp.concatenate(
                    [far[leaf, 2 * k], far[leaf, 2 * k + 1]], axis=1
                )

    lax.fori_loop(0, HELD, fill_rest, 0)
    lax.fori_loop(0, 16, find_places, 0)
    flatten_far()
    gather(0, 0, 16)
    early(0)
    lax.fori_loop(HELD, 16, fill_rest, 0)
    near_of(0, 0)
    near_of(0, 1)
    gather(1, 0, 8)
    mid_a(0)
    gather(1, 8, 12)
    mid_b(0)
    gather(1, 12, 16)
    early(1)
    mid_a(1)
    mid_c(0)
    mid_b(1)
    answer(0, 0, 16)
    near_of(1, 0)
    near_of(1, 1)
    mid_c(1)
    answer(1, 0, 16)
    loads[1].wait()
    v0, v1 = basis[0], basis[1]
    mutual = [jnp.sum(a * b, axis=0, keepdims=True) for a, b in ((v0, v0), (v0, v1), (v1, v1))]
    leaves, sums = [], []
    for p in range(PARTS):
        collect(p)
        span = slice(p * WIDE, (p + 1) * WIDE)
        leaves.append(pltpu.make_async_copy(image.at[p], image_hbm.at[:, pl.ds(p * WIDE, WIDE)], out_sem.at[p]))
        leaves[p].start()
        found = image[p]
        sums.append([jnp.sum(basis[k, :, span] * found, axis=0, keepdims=True) for k in range(2)])
        sums[p].append(jnp.sum(found * found, axis=0, keepdims=True))
    sums = [jnp.concatenate([a, b], axis=1) for a, b in zip(*sums)]
    sums1[group] = jnp.concatenate(sums + mutual + [jnp.zeros((2, COLS), F32)], axis=0)
    for k in range(1, 8):
        remote(sums1.at[group], sums1.at[group], sum_send_sem.at[0], sum_sem.at[0], (z, x, ys[k // 2], cs[k % 2]))
    wait_for(sums1.at[pl.ds(0, 7)], sum_sem.at[0])
    sums2[branch] = jnp.sum(sums1[...], axis=0)
    for k in range(1, 16):
        remote(sums2.at[branch], sums2.at[branch], sum_send_sem.at[1], sum_sem.at[1], (zs[k // 4], xs[k % 4], y, c))
    wait_for(row_send.at[pl.ds(0, DEV - 1)], row_send_sem)
    for p in range(PARTS):
        wait_for(send.at[p, pl.ds(0, DEV - 1)], send_sem.at[p])
        wait_for(reply.at[p, pl.ds(0, DEV - 1)], reply_sem.at[p])
        wait_for(ag0.at[p, 0, three], ag_send_sem.at[p, 0])
        wait_for(ag1.at[p, 0, three], ag_send_sem.at[p, 1])
        wait_for(ag0.at[p, three], ag_send_sem.at[p, 2])
        wait_for(ag1.at[p, three], ag_send_sem.at[p, 3])
        for n in range(4):
            wait_for(par1.at[p, 0, three], par_send_sem.at[p, n])
        wait_for(tops.at[p, pl.ds(0, 7)], top_send_sem.at[p])
    for leave in leaves:
        leave.wait()
    wait_for(sums1.at[pl.ds(0, 7)], sum_send_sem.at[0])
    wait_for(sums2.at[pl.ds(0, 15)], sum_sem.at[1])
    wait_for(sums2.at[pl.ds(0, 15)], sum_send_sem.at[1])
    total = jnp.sum(sums2[...], axis=0) * (1.0 / TOTAL)
    p0, p1, sq = total[0:1], total[1:2], total[2:3]
    m00, m01, m11 = total[3:4], total[4:5], total[5:6]
    square = sq - 2.0 * (p0 * p0 + p1 * p1) + (p0 * p0 * m00 + 2.0 * (p0 * p1) * m01 + p1 * p1 * m11)
    norm = jnp.sqrt(square + 1e-6)
    total_ref[...] = jnp.concatenate([p0, p1, norm, 1.0 / norm, jnp.zeros((4, COLS), F32)], axis=0)


def finish(total_ref, basis, image, out_hbm, hess_ref, out, out_sem):
    p0, p1, scale = total_ref[0:1], total_ref[1:2], total_ref[3:4]
    hess_ref[...] = total_ref[0:3]
    stores = []
    for n in range(ROWS // STEP):
        at = pl.ds(n * STEP, STEP)
        out[at] = (image[at] - (p0 * basis[0, at] + p1 * basis[1, at])) * scale
        stores.append(pltpu.make_async_copy(out.at[at], out_hbm.at[at], out_sem.at[n]))
        stores[n].start()
    for store in stores:
        store.wait()


def body(
    basis, spread_owner, spread_row, spread_weight, gram_term, near_block, near_list,
    leaf_basis, far_block, far_list, ascend, descend, top_block,
):
    vmem = pl.BlockSpec(memory_space=pltpu.VMEM)
    smem = pl.BlockSpec(memory_space=pltpu.SMEM)
    hbm = pl.BlockSpec(memory_space=pl.ANY)
    dma = pltpu.SemaphoreType.DMA
    V = pltpu.VMEM
    image, total = pl.pallas_call(
        kernel,
        out_shape=(
            jax.ShapeDtypeStruct((ROWS, COLS), F32),
            jax.ShapeDtypeStruct((8, COLS), F32),
        ),
        in_specs=[vmem] * 3 + [smem] * 2 + [vmem] + [hbm] * 7,
        out_specs=(hbm, vmem),
        scratch_shapes=[
            V((2, ROWS, COLS), F32), V((2, LEAF, LEAF), BF16), V((2, 8, LEAF, LEAF), BF16),
            V((2, RANK, LEAF), BF16), V((2, 16, RANK, RANK), BF16), V((2, RANK, RANK), BF16),
            V((2, RANK, RANK), BF16),
            V((DEV, ROWS), F32), V((DEV, ROWS), F32), V((DEV, ROWS), F32), V((DEV, ROWS), F32), V((DEV, 128), F32),
            V((DEV, SLOTS, ROWS), BF16), V((DEV, SLOTS, ROWS), BF16),
            V((DEV, SLOTS, 128), F32), V((DEV, SLOTS, 128), F32), V((ROWS, 2 * COLS), BF16),
            V((PARTS, DEV, SLOTS, WIDE), BF16), V((PARTS, DEV, SLOTS, WIDE), BF16),
            V((PARTS, DEV, SLOTS, WIDE), BF16), V((PARTS, DEV, SLOTS, WIDE), BF16),
            V((DEV, 1, 128), F32), V((DEV, 1, 128), F32),
            V((PARTS, ROWS, WIDE), F32), V((PARTS, ROWS, WIDE), F32), V((PARTS, 2, LEAF, WIDE), BF16),
            V((PARTS, ROWS, WIDE), F32), V((PARTS, ROWS, 2 * WIDE), BF16), V((PARTS, ROWS, WIDE), F32),
            V((PARTS, 4, 4, RANK, WIDE), BF16), V((PARTS, 4, 4, RANK, WIDE), BF16), V((32, RANK, WIDE), BF16),
            V((2, RANK, 16 * RANK), BF16), V((16 * RANK, WIDE), BF16),
            V((PARTS, 2, 4, RANK // 2, WIDE), BF16), V((PARTS, 2, 4, RANK // 2, WIDE), BF16),
            V((PARTS, 8, RANK, WIDE), BF16), V((8, 8, COLS), F32), V((16, 8, COLS), F32),
            dma((8,)), dma((PARTS,)), dma((PARTS, 16)), dma, dma((16,)), dma((PARTS,)), dma((PARTS, 16)),
            dma((PARTS, 4)), dma((PARTS, 4)), dma((PARTS, 4)), dma((PARTS, 4)), dma((PARTS,)), dma((PARTS,)),
            dma((2,)), dma((2,)), dma((PARTS,)),
        ],
        compiler_params=pltpu.CompilerParams(
            collective_id=0, has_side_effects=True, vmem_limit_bytes=LIMIT_A
        ),
        name="dual_step",
    )(
        spread_owner.T, spread_row.T, spread_weight.T, near_list, far_list, top_block,
        basis, gram_term, near_block, leaf_basis, far_block, ascend, descend,
    )
    parts = ROWS // STEP
    return tuple(
        pl.pallas_call(
            finish,
            out_shape=(jax.ShapeDtypeStruct((ROWS, COLS), F32), jax.ShapeDtypeStruct((3, COLS), F32)),
            in_specs=[vmem, vmem, vmem],
            out_specs=(hbm, vmem),
            scratch_shapes=[
                V((ROWS, COLS), F32), dma((parts,)),
            ],
            compiler_params=pltpu.CompilerParams(vmem_limit_bytes=LIMIT_B),
            name="finish",
        )(total, basis, image)
    )


def solution(mesh):
    finer = Mesh(mesh.devices.reshape(4, 4, 4, 2), AXES)
    split = P(BRANCH_GROUP)
    return jax.shard_map(
        body,
        mesh=finer,
        in_specs=(
            P(None, BRANCH_GROUP, None), split, split, split, split, split, split,
            split, split, split, split, split, P(GROUP, None),
        ),
        out_specs=(P(BRANCH_GROUP, None), P()),
        check_vma=False,
    )
```
